256 devices in a mesh: rep: 2 (over z), gx: 128 (over y, x, core).
Axes of the slice: x: 8, y: 8, z: 2, core: 2. Of those that a mesh axis runs over, the one named last changes fastest.
The devices are a block of a 8x8x16 slice.
Arguments:
- positions: float32 [3, 1048576], P(None, ('rep', 'gx')), parts along dimension 1, may hold values from 0 to 512, as said below
- polar: float32 [1048576], P(('rep', 'gx')), parts along dimension 0, may hold values from 0.25 to 1
- field_ext: float32 [3, 1048576], P(None, ('rep', 'gx')), parts along dimension 1, may hold values from -10 to 10
- tile_atom: int32 [1048576], P(('rep', 'gx')), parts along dimension 0, may hold values from 0 to 4095, as said below
- tile_list: int32 [8192, 3], P(('rep', 'gx')), parts along dimension 0, may hold values from 0 to 63, as said below
- image_shift: int32 [2, 8192, 3], P(None, ('rep', 'gx')), parts along dimension 1, may hold values from 0 to 1, as said below
Outputs:
- dipoles: float32 [3, 1048576], P(None, ('rep', 'gx')), parts along dimension 1
- residual: float32 [3, 1048576], P(None, ('rep', 'gx')), parts along dimension 1
The draws below stay inside these ranges and needn't reach their ends.
There are 2 independent parts, one for each index of `rep`. The reference program is written for one: setup_inputs(seed, part) draws one part's arguments, and reference() takes and returns one part's arrays. A program takes and returns all parts, laid end to end along the dimension named above; each array names one. Nothing has to cross between parts.
Inputs may be any that keep to these rules, and one draw needn't show every extreme that they name: `positions`: coordinates lie in a box of 512 by 128 by 64; the atoms of slab s have first coordinate between 4 s and 4 s + 4; no two atoms, and no atom and a periodic image of another, are closer than 1.4. `tile_atom`: for each slab, a permutation of 0 to 4095. `tile_list`: entry 0 of a tile is the tile's own index within its slab. Entry n of a tile of slab s names tile n of slab s if n < 32, else tile n - 32 of slab s + 1 (slab 0 after the last). `image_shift`: offsets along the second and third coordinates in box lengths, one pair for each entry of tile_list; zero for entry 0.
All inputs are finite; a program needn't handle non-finite values.
Results may differ from the reference program's by a relative error of at most 0.0003.
Values sent between devices are 32-bit elements; how exact they have to be, the bound alone decides.
A program may use at most 64 MiB of HBM per device.

```python
import math
import jax
import jax.numpy as jnp
from jax import lax

TILE = 128
TILES_DEV = 32
NB = 3
ITERS = 4
TILES = 4096
ATOMS_DEV = 4096
ATOMS = 524288


def atom_order(key):
    slab_count = ATOMS // ATOMS_DEV
    keys = jax.random.split(jax.random.fold_in(key, 11), slab_count)

    def one_slab(slab_key):
        return jax.random.permutation(slab_key, ATOMS_DEV).astype(jnp.int32)
    return jax.vmap(one_slab)(keys).reshape(ATOMS)


def lattice_places():
    slot_ids = jnp.arange(ATOMS, dtype=jnp.int32)
    slab_ids = slot_ids // ATOMS_DEV
    local_ids = slot_ids % ATOMS_DEV
    tile_ids = local_ids // TILE
    within = local_ids % TILE
    rows_z = TILES_DEV // 8
    cell_y = tile_ids // rows_z
    cell_z = tile_ids % rows_z
    layer_id = within // 64
    along_y = within // 8 % 8
    along_z = within % 8
    coord_x = 4 * slab_ids + 2 * layer_id + 1
    coord_y = 2 * (8 * cell_y + along_y) + 1
    coord_z = 2 * (8 * cell_z + along_z) + 1
    return (jnp.stack([coord_x, coord_y, coord_z]).astype(jnp.float32), slab_ids)


def draw_tile_atom(key, part):
    return atom_order(key)


def draw_positions(key, part):
    order_ids = atom_order(key)
    base, slab_ids = lattice_places()
    jitter_key = jax.random.fold_in(key, 23)
    jitter = jax.random.uniform(jitter_key, (3, ATOMS), jnp.float32, -0.3, 0.3)
    placed = base + jitter
    target = slab_ids * ATOMS_DEV + order_ids
    return jnp.zeros((3, ATOMS), jnp.float32).at[:, target].set(placed)


def draw_field_ext(key, part):
    slab_count = ATOMS // ATOMS_DEV
    slab_ids = jnp.arange(ATOMS, dtype=jnp.int32) // ATOMS_DEV
    ramp = slab_ids.astype(jnp.float32) / (slab_count - 1)
    noise = jnp.clip(jax.random.normal(key, (3, ATOMS), jnp.float32), -5.0, 5.0)
    return noise * (0.6 + 1.2 * ramp)


def neighbour_entries(key):
    score_key = jax.random.fold_in(key, 37)
    scores = jax.random.randint(score_key, (TILES, 7), 0, 1 << 20) * 8 + jnp.arange(7, dtype=jnp.int32)[None, :]
    picked = jnp.argsort(scores, axis=1)[:, :NB - 1].astype(jnp.int32) + 1
    step_x = picked // 4
    step_y = picked // 2 % 2
    step_z = picked % 2
    rows_z = TILES_DEV // 8
    tile_ids = jnp.arange(TILES, dtype=jnp.int32) % TILES_DEV
    cell_y = (tile_ids // rows_z)[:, None]
    cell_z = (tile_ids % rows_z)[:, None]
    next_y = cell_y + step_y
    next_z = cell_z + step_z
    image_y = next_y // 8
    image_z = next_z // rows_z
    named = step_x * TILES_DEV + next_y % 8 * rows_z + next_z % rows_z
    lists = jnp.concatenate([tile_ids[:, None], named], axis=1).astype(jnp.int32)
    zeros_col = jnp.zeros((TILES, 1), jnp.int32)
    shifts = jnp.stack([jnp.concatenate([zeros_col, image_y], axis=1), jnp.concatenate([zeros_col, image_z], axis=1)]).astype(jnp.int32)
    return (lists, shifts)


def draw_tile_list(key, part):
    lists, shifts = neighbour_entries(key)
    return lists


def draw_image_shift(key, part):
    lists, shifts = neighbour_entries(key)
    return shifts


def shard_levels(own_key, shape, cuts, least, largest):
    factor_of = 1.0
    for position, blocks in cuts:
        steps = jax.random.uniform(jax.random.fold_in(jax.random.fold_in(own_key, 6), position), (blocks,), jnp.float32, least / len(cuts), largest / len(cuts))
        factor_of = factor_of * jnp.repeat(jnp.exp(steps), shape[position] // blocks).reshape((-1,) + (1,) * (len(shape) - 1 - position))
    return factor_of


def setup_inputs(seed: int = 0, part: int = 0) -> dict:
    splits = jax.random.split(jax.random.key(seed), 7)
    part_splits = jax.random.split(jax.random.fold_in(splits[6], part), 7)
    positions = draw_positions(jax.random.fold_in(jax.random.fold_in(splits[6], part), 71), part)
    polar = jnp.clip(jnp.exp(math.log(1.0) - 1.3862944 * jax.random.uniform(part_splits[1], (ATOMS,), jnp.float32) ** shard_levels(part_splits[1], (ATOMS,), ((0, 128),), -0.2, 0.2)), 0.25, 1.0)
    field_ext = draw_field_ext(jax.random.fold_in(jax.random.fold_in(splits[6], part), 71), part)
    tile_atom = draw_tile_atom(jax.random.fold_in(jax.random.fold_in(splits[6], part), 71), part)
    tile_list = draw_tile_list(jax.random.fold_in(jax.random.fold_in(splits[6], part), 71), part)
    image_shift = draw_image_shift(jax.random.fold_in(jax.random.fold_in(splits[6], part), 71), part)
    return {"positions": positions, "polar": polar, "field_ext": field_ext, "tile_atom": tile_atom, "tile_list": tile_list, "image_shift": image_shift}


thole_factor = 0.39

def pair_block(place_left, root_left, moment_left, place_right, root_right, moment_right, weights, self_flags):
    offset_x = place_right[:, 0, None, :] - place_left[:, 0, :, None]
    offset_y = place_right[:, 1, None, :] - place_left[:, 1, :, None]
    offset_z = place_right[:, 2, None, :] - place_left[:, 2, :, None]
    dist_sq = offset_x * offset_x + offset_y * offset_y + offset_z * offset_z
    tile_width = place_left.shape[2]
    row_ids = lax.broadcasted_iota(jnp.int32, (tile_width, tile_width), 0)
    column_ids = lax.broadcasted_iota(jnp.int32, (tile_width, tile_width), 1)
    same_atom = jnp.logical_and(self_flags[:, None, None] > 0, (row_ids == column_ids)[None])
    dist_sq = jnp.where(same_atom, 1.0, dist_sq)
    inv_dist = lax.rsqrt(dist_sq)
    distance = dist_sq * inv_dist
    damp_arg = thole_factor * dist_sq * distance / (root_left[:, :, None] * root_right[:, None, :])
    decay = jnp.exp(-damp_arg)
    inv_cube = jnp.where(same_atom, 0.0, weights[:, None, None] * inv_dist * inv_dist * inv_dist)
    coeff_three = (1.0 - decay) * inv_cube
    coeff_five = 3.0 * (1.0 - (1.0 + damp_arg) * decay) * inv_cube * inv_dist * inv_dist
    offsets = (offset_x, offset_y, offset_z)
    proj_right = offset_x * moment_right[:, 0, None, :] + offset_y * moment_right[:, 1, None, :] + offset_z * moment_right[:, 2, None, :]
    proj_left = offset_x * moment_left[:, 0, :, None] + offset_y * moment_left[:, 1, :, None] + offset_z * moment_left[:, 2, :, None]
    lift_right = coeff_five * proj_right
    lift_left = coeff_five * proj_left
    field_left = jnp.stack([lax.optimization_barrier(jnp.sum(lift_right * offsets[component] - coeff_three * moment_right[:, component, None, :], axis=2)) for component in range(3)], axis=1)
    field_right = jnp.stack([lax.optimization_barrier(jnp.sum(lift_left * offsets[component] - coeff_three * moment_left[:, component, :, None], axis=1)) for component in range(3)], axis=1)
    return (field_left, field_right)

def slab_fields(window_place, window_root, window_moment, left_index, right_index, image_vec, weights, self_flags):
    entries = left_index.shape[0]
    block_size = math.gcd(entries, 32)
    window_size = window_place.shape[0]
    tile_width = window_place.shape[2]
    slot_ids = jnp.arange(window_size, dtype=jnp.int32)

    def accumulate(summed, first_entry):
        left_rows = lax.dynamic_slice_in_dim(left_index, first_entry, block_size)
        right_rows = lax.dynamic_slice_in_dim(right_index, first_entry, block_size)
        image_rows = lax.dynamic_slice_in_dim(image_vec, first_entry, block_size)
        weight_rows = lax.dynamic_slice_in_dim(weights, first_entry, block_size)
        flag_rows = lax.dynamic_slice_in_dim(self_flags, first_entry, block_size)
        place_left = jnp.take(window_place, left_rows, axis=0)
        place_right = jnp.take(window_place, right_rows, axis=0) + image_rows[:, :, None]
        field_left, field_right = pair_block(place_left, jnp.take(window_root, left_rows, axis=0), jnp.take(window_moment, left_rows, axis=0), place_right, jnp.take(window_root, right_rows, axis=0), jnp.take(window_moment, right_rows, axis=0), weight_rows, flag_rows)
        hit_left = (left_rows[:, None] == slot_ids[None, :]).astype(jnp.float32)
        hit_right = (right_rows[:, None] == slot_ids[None, :]).astype(jnp.float32)
        summed = summed + jnp.einsum('ew,ef->wf', hit_left, field_left.reshape(block_size, 3 * tile_width), precision=lax.Precision.HIGHEST)
        summed = summed + jnp.einsum('ew,ef->wf', hit_right, field_right.reshape(block_size, 3 * tile_width), precision=lax.Precision.HIGHEST)
        return (summed, None)
    first_entries = jnp.arange(0, entries, block_size, dtype=jnp.int32)
    summed, _ = lax.scan(accumulate, jnp.zeros((window_size, 3 * tile_width), jnp.float32), first_entries)
    return summed.reshape(window_size, 3, tile_width)

def image_vectors(lists, shifts, last_flag, tile_count, box_x, box_y, box_z):
    crossing = lists >= tile_count
    wrapped = jnp.where(jnp.logical_and(crossing, last_flag), box_x, 0.0)
    vectors = jnp.stack([wrapped, shifts[0].astype(jnp.float32) * box_y, shifts[1].astype(jnp.float32) * box_z], axis=-1)
    return vectors.reshape(-1, 3)

def reference(positions, polar, field_ext, tile_atom, tile_list, image_shift):
    slab_count = TILES // TILES_DEV
    slot_atom = jnp.arange(ATOMS, dtype=jnp.int32) // ATOMS_DEV * ATOMS_DEV + tile_atom
    tiled_place = positions[:, slot_atom].reshape(3, TILES, TILE).transpose(1, 0, 2)
    tiled_polar = polar[slot_atom].reshape(TILES, TILE)
    tiled_root = jnp.sqrt(tiled_polar)
    tiled_rhs = field_ext[:, slot_atom].reshape(3, TILES, TILE).transpose(1, 0, 2)
    box_x = 4.0 * slab_count
    box_y = 128.0
    box_z = 2.0 * TILES_DEV
    last_flag = (jnp.arange(TILES, dtype=jnp.int32) // TILES_DEV == slab_count - 1)[:, None]
    image_all = image_vectors(tile_list, image_shift, last_flag, TILES_DEV, box_x, box_y, box_z)
    entry_ids = jnp.arange(NB, dtype=jnp.int32)
    own_left = jnp.repeat(jnp.arange(TILES_DEV, dtype=jnp.int32), NB)
    own_weights = jnp.tile(jnp.where(entry_ids == 0, 0.5, 1.0), TILES_DEV)
    own_self = jnp.tile((entry_ids == 0).astype(jnp.int32), TILES_DEV)
    slab_ids = jnp.arange(slab_count, dtype=jnp.int32)

    def apply_operator(moment):

        def per_slab(summed, slab):
            first = slab * TILES_DEV
            after = (slab + 1) % slab_count * TILES_DEV
            window_place = jnp.concatenate([lax.dynamic_slice_in_dim(tiled_place, first, TILES_DEV), lax.dynamic_slice_in_dim(tiled_place, after, TILES_DEV)], axis=0)
            window_root = jnp.concatenate([lax.dynamic_slice_in_dim(tiled_root, first, TILES_DEV), lax.dynamic_slice_in_dim(tiled_root, after, TILES_DEV)], axis=0)
            window_moment = jnp.concatenate([lax.dynamic_slice_in_dim(moment, first, TILES_DEV), lax.dynamic_slice_in_dim(moment, after, TILES_DEV)], axis=0)
            lists = lax.dynamic_slice_in_dim(tile_list, first, TILES_DEV).reshape(-1)
            images = lax.dynamic_slice_in_dim(image_all, first * NB, TILES_DEV * NB)
            window = slab_fields(window_place, window_root, window_moment, own_left, lists, images, own_weights, own_self)
            summed = lax.dynamic_update_slice_in_dim(summed, lax.dynamic_slice_in_dim(summed, first, TILES_DEV) + window[:TILES_DEV], first, 0)
            summed = lax.dynamic_update_slice_in_dim(summed, lax.dynamic_slice_in_dim(summed, after, TILES_DEV) + window[TILES_DEV:], after, 0)
            return (summed, None)
        fields, _ = lax.scan(per_slab, jnp.zeros((TILES, 3, TILE), jnp.float32), slab_ids)
        return moment / tiled_polar[:, None, :] - fields
    solution = jnp.zeros_like(tiled_rhs)
    resid = tiled_rhs
    direction = tiled_rhs
    norm_now = jnp.sum(resid * resid)
    for iteration in range(ITERS):
        applied = apply_operator(direction)
        step_size = norm_now / jnp.sum(direction * applied)
        solution = solution + step_size * direction
        resid = resid - step_size * applied
        norm_next = jnp.sum(resid * resid)
        direction = resid + norm_next / norm_now * direction
        norm_now = norm_next
    dipoles = jnp.zeros((3, ATOMS), jnp.float32).at[:, slot_atom].set(solution.transpose(1, 0, 2).reshape(3, ATOMS))
    residual = jnp.zeros((3, ATOMS), jnp.float32).at[:, slot_atom].set(resid.transpose(1, 0, 2).reshape(3, ATOMS))
    return (dipoles, residual)
```

```python
import functools

import jax
import jax.numpy as jnp
from jax import lax
from jax.experimental import pallas as pl
from jax.experimental.pallas import tpu as pltpu
from jax.sharding import PartitionSpec as P

ITERS = 4
MESH = pl.DeviceIdType.MESH
THOLE = 0.39
F32 = jnp.float32
ROWS = 8


def lanes(index):
    return slice(index * 128, (index + 1) * 128)


def tiled_order_kernel(pos_ref, polar_ref, field_ref, atom_ref, pack_ref, inv_alpha_ref, rhs_ref, slot_ref):
    tiles = atom_ref.shape[0]
    atom = atom_ref[...]
    high = atom // 128
    low = atom % 128

    def pick(step, found):
        hit = high == step
        cols = pl.ds(pl.multiple_of(step * 128, 128), 128)
        rows = [pos_ref[c : c + 1, cols] for c in range(3)]
        rows += [field_ref[c : c + 1, cols] for c in range(3)]
        rows.append(polar_ref[pl.ds(step, 1), :])
        new = []
        for row, old in zip(rows, found):
            wide = jnp.broadcast_to(row, (tiles, 128))
            new.append(jnp.where(hit, jnp.take_along_axis(wide, low, axis=1), old))
        return tuple(new)

    zero = jnp.zeros((tiles, 128), F32)
    found = lax.fori_loop(0, tiles, pick, (zero,) * 7)
    for c in range(3):
        pack_ref[c * tiles : (c + 1) * tiles, :] = found[c]
        rhs_ref[c * tiles : (c + 1) * tiles, :] = found[3 + c]
    pack_ref[3 * tiles : 4 * tiles, :] = lax.rsqrt(found[6])
    inv_alpha_ref[...] = 1.0 / found[6]

    high_ids = lax.broadcasted_iota(jnp.int32, (tiles, 128), 0)
    low_ids = lax.broadcasted_iota(jnp.int32, (128, 128), 0)
    lane_ids = lax.broadcasted_iota(jnp.int32, (tiles, 128), 1).astype(F32)

    def invert(step, total):
        row = atom_ref[pl.ds(step, 1), :]
        hot_high = high_ids == row // 128
        hot_low = jnp.where(low_ids == row % 128, 1.0, 0.0).astype(jnp.bfloat16)
        left = jnp.concatenate(
            [
                jnp.where(hot_high, lax.convert_element_type(step, F32), 0.0),
                jnp.where(hot_high, lane_ids, 0.0),
            ],
            axis=0,
        ).astype(jnp.bfloat16)
        return total + lax.dot_general(
            left, hot_low, (((1,), (1,)), ((), ())), preferred_element_type=F32
        )

    total = lax.fori_loop(0, tiles, invert, jnp.zeros((2 * tiles, 128), F32))
    slot_ref[...] = (total[:tiles] * 128.0 + total[tiles:]).astype(jnp.int32)


def atom_order_kernel(x_ref, r_ref, slot_ref, dipoles_ref, residual_ref):
    tiles = slot_ref.shape[0]
    slot = slot_ref[...]
    high = slot // 128
    low = slot % 128

    def pick(step, found):
        hit = high == step
        rows = [ref[pl.ds(c * tiles + step, 1), :] for ref in (x_ref, r_ref) for c in range(3)]
        new = []
        for row, old in zip(rows, found):
            wide = jnp.broadcast_to(row, (tiles, 128))
            new.append(jnp.where(hit, jnp.take_along_axis(wide, low, axis=1), old))
        return tuple(new)

    zero = jnp.zeros((tiles, 128), F32)
    found = lax.fori_loop(0, tiles, pick, (zero,) * 6)
    for c in range(3):
        for h in range(tiles):
            dipoles_ref[c : c + 1, lanes(h)] = found[c][h : h + 1, :]
            residual_ref[c : c + 1, lanes(h)] = found[3 + c][h : h + 1, :]


def pair_tensor(left, right, diagonal):
    dx = right[0] - left[0]
    dy = right[1] - left[1]
    dz = right[2] - left[2]
    square = dx * dx + dy * dy + dz * dz
    if diagonal is not None:
        square = jnp.where(diagonal, 1.0, square)
    inv = lax.rsqrt(square)
    minus_u = square * (square * inv) * (left[3] * right[3])
    decay = jnp.exp(minus_u)
    inv_square = inv * inv
    inv_cube = inv * inv_square
    if diagonal is not None:
        inv_cube = jnp.where(diagonal, 0.0, inv_cube)
    rest = 1.0 - decay
    g3 = rest * inv_cube
    g5 = (rest + minus_u * decay) * inv_cube * (3.0 * inv_square)
    ax = g5 * dx
    ay = g5 * dy
    return (
        ax * dx - g3,
        ax * dy,
        ax * dz,
        ay * dy - g3,
        ay * dz,
        g5 * dz * dz - g3,
    )


def times(t, m):
    return (
        t[0] * m[0] + t[1] * m[1] + t[2] * m[2],
        t[1] * m[0] + t[3] * m[1] + t[4] * m[2],
        t[2] * m[0] + t[4] * m[1] + t[5] * m[2],
    )


def solve_kernel(
    group,
    inner,
    pack_ref,
    rhs_ref,
    inv_alpha_ref,
    list_ref,
    shift_ref,
    x_ref,
    r_ref,
    own_t,
    pair_t,
    part,
    cols_a,
    cols_b,
    win_p,
    win_0,
    win_1,
    win_2,
    win_3,
    top,
    ret_out,
    ret_in,
    right_rows,
    hot,
    colmat,
    gram,
    sums_1,
    sums_2,
    ring_send,
    ring_recv,
    sum_send,
    sum_recv,
):
    tiles = rhs_ref.shape[0] // 3
    me = lax.axis_index("gx")
    outer = group // inner
    row, col = me // inner, me % inner
    after = lax.rem(me + 1, group)
    before = lax.rem(me + group - 1, group)
    peers_1 = [row * inner + lax.rem(col + d, inner) for d in range(1, inner)]
    peers_2 = [lax.rem(row + d, outer) * inner + col for d in range(1, outer)]
    wins = (win_0, win_1, win_2, win_3)

    barrier = pltpu.get_barrier_semaphore()
    everyone = [after, before] + peers_1 + peers_2
    for peer in everyone:
        pl.semaphore_signal(barrier, inc=1, device_id={"gx": peer}, device_id_type=MESH)

    def ring_copy(src, dst, index, peer):
        return pltpu.make_async_remote_copy(
            src_ref=src,
            dst_ref=dst,
            send_sem=ring_send.at[index],
            recv_sem=ring_recv.at[index],
            device_id={"gx": peer},
            device_id_type=MESH,
        )

    def sum_copies(which, stage):
        buf = sums_1 if stage == 0 else sums_2
        at = col if stage == 0 else row
        peers = peers_1 if stage == 0 else peers_2
        base = which * (inner + outer) + stage * inner
        return [
            pltpu.make_async_remote_copy(
                src_ref=buf.at[which, at],
                dst_ref=buf.at[which, at],
                send_sem=sum_send.at[base + d],
                recv_sem=sum_recv.at[base + d],
                device_id={"gx": peer},
                device_id_type=MESH,
            )
            for d, peer in enumerate(peers)
        ]

    def sum_start(which, stage, value):
        buf = sums_1 if stage == 0 else sums_2
        buf[which, pl.ds(col if stage == 0 else row, 1)] = value[None]
        for copy in sum_copies(which, stage):
            copy.start()

    def sum_finish(which, stage):
        for copy in sum_copies(which, stage):
            copy.wait()
        buf = sums_1 if stage == 0 else sums_2
        total = buf[which, 0]
        for d in range(1, inner if stage == 0 else outer):
            total = total + buf[which, d]
        return total

    def inner_rows(a, b):
        return jnp.sum(a * b, axis=0, keepdims=True)

    sub_ids = lax.broadcasted_iota(jnp.int32, (16, 128), 0)
    lane_ids = lax.broadcasted_iota(jnp.int32, (16, 128), 1)

    def packed_sums(stack):
        totals = jnp.sum(stack, axis=1, keepdims=True)
        return jnp.sum(jnp.where(sub_ids == lane_ids, totals, 0.0), axis=0, keepdims=True)

    def unpacked(sums):
        gram[...] = jnp.broadcast_to(sums, (128, 128)).T

    rhs = rhs_ref[...]
    inv_alpha = inv_alpha_ref[...]
    inv_alpha_3 = jnp.concatenate([inv_alpha] * 3, axis=0)
    win_p[0 : 4 * tiles, :] = pack_ref[...]
    win_0[0 : 3 * tiles, :] = rhs
    colmat[...] = jnp.zeros((128, 128), F32)
    gram[...] = jnp.zeros((128, 128), F32)
    gram[0:1, :] = inner_rows(rhs, rhs)
    gram[1:2, :] = inner_rows(rhs, rhs * inv_alpha_3)

    def spread(buf, ref, index, count):
        for c in range(count):
            line = ref[pl.ds(c * tiles + index, 1), :]
            buf[c] = jnp.broadcast_to(line, (128, 128)).T

    def right_lines(n, vector):
        first = n + jnp.where(n >= tiles, 3 * tiles, 0)
        lines = [win_p[pl.ds(first + c * tiles, 1), :] for c in range(4)]
        if vector is not None:
            lines = [lines[c] + vector[c] for c in range(3)] + lines[3:]
        lines[3] = lines[3] * (-THOLE)
        return [jnp.broadcast_to(line, (ROWS, 128)) for line in lines]

    block_sub = lax.broadcasted_iota(jnp.int32, (ROWS, 128), 0)
    block_lane = lax.broadcasted_iota(jnp.int32, (ROWS, 128), 1)
    steps = 128 // ROWS

    def rows_of(i):
        return pl.ds(pl.multiple_of(i * ROWS, ROWS), ROWS)

    def own_tensors(t, cols):
        right = right_lines(t, None)

        def block(i, carry):
            left = [cols[c, rows_of(i), :] for c in range(4)]
            same = block_sub + i * ROWS == block_lane
            for k, value in enumerate(pair_tensor(left, right, same)):
                own_t[t, k, rows_of(i), :] = value
            return carry

        lax.fori_loop(0, steps, block, 0, unroll=True)

    last = me == group - 1

    def pair_tensors(t, cols):
        for e in range(2):
            n = list_ref[t, e + 1]
            wrap = jnp.where(jnp.logical_and(n >= tiles, last), 4.0 * group, 0.0)
            vector = (
                wrap,
                shift_ref[0, t, e + 1].astype(F32) * 128.0,
                shift_ref[1, t, e + 1].astype(F32) * (2.0 * tiles),
            )
            right = right_lines(n, vector)

            def block(i, carry):
                left = [cols[c, rows_of(i), :] for c in range(4)]
                for k, value in enumerate(pair_tensor(left, right, None)):
                    pair_t[t, e, k, rows_of(i), :] = value
                return carry

            lax.fori_loop(0, steps, block, 0, unroll=True)

    def in_pairs(ref, count, work):
        spread(cols_a, ref, 0, count)

        def body(u, carry):
            t = 2 * u
            spread(cols_b, ref, t + 1, count)
            work(t, cols_a)
            spread(cols_a, ref, lax.rem(t + 2, tiles), count)
            work(t + 1, cols_b)
            return carry

        lax.fori_loop(0, tiles // 2, body, 0)

    def own_fields(win):
        def body(t, carry):
            m = [
                jnp.broadcast_to(win[pl.ds(c * tiles + t, 1), :], (ROWS, 128))
                for c in range(3)
            ]

            def block(i, inside):
                tensor = [own_t[t, k, rows_of(i), :] for k in range(6)]
                for c, value in enumerate(times(tensor, m)):
                    part[t, c, rows_of(i), :] = value
                return inside

            lax.fori_loop(0, steps, block, 0, unroll=True)
            return carry

        lax.fori_loop(0, tiles, body, 0)

    def right_fields(win):
        def work(t, cols):
            def block(i, sums):
                m = [cols[c, rows_of(i), :] for c in range(3)]
                new = []
                for e in range(2):
                    tensor = [pair_t[t, e, k, rows_of(i), :] for k in range(6)]
                    new += list(times(tensor, m))
                return tuple(a + b for a, b in zip(sums, new))

            sums = lax.fori_loop(0, steps, block, (jnp.zeros((ROWS, 128), F32),) * 6, unroll=True)
            for e in range(2):
                for c in range(3):
                    right_rows[pl.ds(2 * tiles * c + 2 * t + e, 1), :] = jnp.sum(
                        sums[3 * e + c], axis=0, keepdims=True
                    )

        in_pairs(win, 3, work)
        rows = right_rows[...]
        rows = jnp.concatenate(
            [rows[2 * tiles * c : 2 * tiles * (c + 1)] for c in range(3)], axis=1
        )
        first = rows.astype(jnp.bfloat16)
        rows = rows - first.astype(F32)
        second = rows.astype(jnp.bfloat16)
        third = (rows - second.astype(F32)).astype(jnp.bfloat16)
        split = jnp.concatenate([first, second, third], axis=0)
        total = jnp.dot(hot[...], split, preferred_element_type=F32)
        return [
            jnp.concatenate([half[:, lanes(c)] for c in range(3)], axis=0)
            for half in (total[0:tiles], total[tiles : 2 * tiles])
        ]

    full_lane = lax.broadcasted_iota(jnp.int32, (128, 128), 1)

    def gather_column(t):
        now = colmat[...]
        for c in range(3):
            total = jnp.sum(part[t, c], axis=1, keepdims=True)
            now = jnp.where(full_lane == c * tiles + t, total, now)
        colmat[...] = now

    def left_fields(win):
        def body(t, carry):
            gather_column(lax.rem(t + tiles - 1, tiles))
            m = []
            for e in range(2):
                n = list_ref[t, e + 1]
                first = n + jnp.where(n >= tiles, 2 * tiles, 0)
                m.append(
                    [
                        jnp.broadcast_to(win[pl.ds(first + c * tiles, 1), :], (ROWS, 128))
                        for c in range(3)
                    ]
                )

            def block(i, inside):
                sums = [part[t, c, rows_of(i), :] for c in range(3)]
                for e in range(2):
                    tensor = [pair_t[t, e, k, rows_of(i), :] for k in range(6)]
                    sums = [a + b for a, b in zip(sums, times(tensor, m[e]))]
                for c in range(3):
                    part[t, c, rows_of(i), :] = sums[c]
                return inside

            lax.fori_loop(0, steps, block, 0, unroll=True)
            return carry

        lax.fori_loop(0, tiles, body, 0)
        gather_column(tiles - 1)
        return colmat[...].T[0 : 3 * tiles]

    in_pairs(pack_ref, 4, own_tensors)

    pl.semaphore_wait(barrier, len(everyone))
    halo_p = ring_copy(pack_ref, win_p.at[4 * tiles : 8 * tiles], 0, before)
    halo_p.start()
    halos = [ring_copy(rhs_ref, win_0.at[3 * tiles : 6 * tiles], 1, before)]
    halos += [
        ring_copy(wins[k].at[0 : 3 * tiles], wins[k].at[3 * tiles : 6 * tiles], 1 + k, before)
        for k in range(1, ITERS)
    ]
    returns = [
        ring_copy(ret_out.at[k], ret_in.at[k], 1 + ITERS + k, after) for k in range(ITERS)
    ]
    halos[0].start()
    sum_start(0, 0, packed_sums(gram[0:16, :]))

    own_fields(win_0)

    hot_lane = lax.broadcasted_iota(jnp.int32, (1, 128), 1)

    def mark(t, carry):
        for e in range(2):
            value = jnp.where(hot_lane == list_ref[t, e + 1], 1.0, 0.0)
            gram[pl.ds(2 * t + e, 1), :] = value
        return carry

    lax.fori_loop(0, tiles, mark, 0)
    marks = gram[...].T[0 : 2 * tiles, 0 : 2 * tiles].astype(jnp.bfloat16)
    hot[...] = jnp.concatenate([marks] * 3, axis=1)
    gram[...] = jnp.zeros((128, 128), F32)

    sum_start(0, 1, sum_finish(0, 0))
    halo_p.wait()
    in_pairs(pack_ref, 4, pair_tensors)

    vectors = [rhs]
    pair_index = {}
    centre = None
    centre_row = None
    for k in range(ITERS):
        if k > 0:
            halos[k].start()
        kept, sent = right_fields(wins[k])
        ret_out[k] = sent
        if k > 0:
            own_fields(wins[k])
        returns[k].start()
        halos[k].wait()
        field = left_fields(wins[k])
        field = field + kept
        if k == 0:
            unpacked(sum_finish(0, 1))
            centre_row = gram[1:2, :] / gram[0:1, :]
            gram[...] = jnp.zeros((128, 128), F32)
            gram[0:1, :] = inner_rows(rhs, rhs)
            pair_index[(0, 0)] = 0
            shifted = jnp.concatenate([inv_alpha - centre_row] * 3, axis=0)
        returns[k].wait()
        now = vectors[k]
        new = shifted * now - (field + ret_in[k])
        if k + 1 < ITERS:
            wins[k + 1][0 : 3 * tiles, :] = new
        else:
            top[...] = new
        vectors = []
        for j in range(k + 2):
            if j == ITERS:
                vectors.append(top[...])
            else:
                vectors.append(rhs_ref[...] if j == 0 else wins[j][0 : 3 * tiles, :])
        for j in range(k + 2):
            pair_index[(j, k + 1)] = len(pair_index)
            index = pair_index[(j, k + 1)]
            gram[index : index + 1, :] = inner_rows(vectors[j], new)

    sum_start(1, 0, packed_sums(gram[0:16, :]))
    sum_start(1, 1, sum_finish(1, 0))
    unpacked(sum_finish(1, 1))

    def entry(a, b):
        index = pair_index[(min(a, b), max(a, b))]
        return gram[index : index + 1, :]

    def form(a, b):
        out = None
        for i, p in enumerate(a):
            for j, q in enumerate(b):
                term = p * q * entry(i, j)
                out = term if out is None else out + term
        return out

    def plus(a, scale, b):
        out = []
        for i in range(max(len(a), len(b))):
            term = scale * b[i] if i < len(b) else None
            if i < len(a):
                out.append(a[i] if term is None else a[i] + term)
            else:
                out.append(term)
        return out

    one = jnp.ones((1, 128), F32)
    x_coef = []
    r_coef = [one]
    d_coef = [one]
    norm_now = form(r_coef, r_coef)
    for iteration in range(ITERS):
        applied = [centre_row * v for v in d_coef] + [0.0 * one]
        applied = [
            applied[i] + d_coef[i - 1] if i > 0 else applied[i] for i in range(len(applied))
        ]
        step = norm_now / form(d_coef, applied)
        x_coef = plus(x_coef, step, d_coef)
        r_coef = plus(r_coef, -step, applied)
        if iteration + 1 < ITERS:
            norm_next = form(r_coef, r_coef)
            d_coef = plus(r_coef, norm_next / norm_now, d_coef)
            norm_now = norm_next

    for out_ref, coef in ((x_ref, x_coef), (r_ref, r_coef)):
        total = None
        for j, value in enumerate(coef):
            term = value * vectors[j]
            total = term if total is None else total + term
        out_ref[...] = total


def on_device(group, positions, polar, field_ext, tile_atom, tile_list, image_shift):
    atoms = tile_atom.shape[0]
    tiles = tile_list.shape[0]
    inner = 16 if group % 16 == 0 else 2
    outer = group // inner
    vmem = pl.BlockSpec(memory_space=pltpu.VMEM)
    smem = pl.BlockSpec(memory_space=pltpu.SMEM)
    state = jax.ShapeDtypeStruct((3 * tiles, 128), F32)

    def shape(*dims, dtype=F32):
        return jax.ShapeDtypeStruct(dims, dtype)

    pack, inv_alpha, rhs, slot = pl.pallas_call(
        tiled_order_kernel,
        out_shape=(shape(4 * tiles, 128), shape(tiles, 128), state, shape(tiles, 128, dtype=jnp.int32)),
        in_specs=[vmem] * 4,
        out_specs=(vmem,) * 4,
        name="tiled_order",
    )(positions, polar.reshape(tiles, 128), field_ext, tile_atom.reshape(tiles, 128))

    sum_count = 2 * (inner + outer)
    ring_count = 1 + 2 * ITERS
    x, r = pl.pallas_call(
        functools.partial(solve_kernel, group, inner),
        out_shape=(state, state),
        in_specs=[vmem] * 3 + [smem] * 2,
        out_specs=(vmem,) * 2,
        scratch_shapes=[
            pltpu.VMEM((tiles, 6, 128, 128), F32),
            pltpu.VMEM((tiles, 2, 6, 128, 128), F32),
            pltpu.VMEM((tiles, 3, 128, 128), F32),
            pltpu.VMEM((4, 128, 128), F32),
            pltpu.VMEM((4, 128, 128), F32),
            pltpu.VMEM((8 * tiles, 128), F32),
        ]
        + [pltpu.VMEM((6 * tiles, 128), F32)] * ITERS
        + [
            pltpu.VMEM((3 * tiles, 128), F32),
            pltpu.VMEM((ITERS, 3 * tiles, 128), F32),
            pltpu.VMEM((ITERS, 3 * tiles, 128), F32),
            pltpu.VMEM((6 * tiles, 128), F32),
            pltpu.VMEM((2 * tiles, 6 * tiles), jnp.bfloat16),
            pltpu.VMEM((128, 128), F32),
            pltpu.VMEM((128, 128), F32),
            pltpu.VMEM((2, inner, 1, 128), F32),
            pltpu.VMEM((2, outer, 1, 128), F32),
            pltpu.SemaphoreType.DMA((ring_count,)),
            pltpu.SemaphoreType.DMA((ring_count,)),
            pltpu.SemaphoreType.DMA((sum_count,)),
            pltpu.SemaphoreType.DMA((sum_count,)),
        ],
        compiler_params=pltpu.CompilerParams(
            collective_id=0, has_side_effects=True, vmem_limit_bytes=60 * 1024 * 1024
        ),
        name="solve",
    )(pack, rhs, inv_alpha, tile_list, image_shift)

    return pl.pallas_call(
        atom_order_kernel,
        out_shape=(shape(3, atoms), shape(3, atoms)),
        in_specs=[vmem] * 3,
        out_specs=(vmem,) * 2,
        name="atom_order",
    )(x, r, slot)


def solution(mesh):
    both = ("rep", "gx")
    return jax.shard_map(
        functools.partial(on_device, mesh.shape["gx"]),
        mesh=mesh,
        in_specs=(
            P(None, both),
            P(both),
            P(None, both),
            P(both),
            P(both, None),
            P(None, both, None),
        ),
        out_specs=(P(None, both), P(None, both)),
        check_vma=False,
    )
```

```python
import functools

import jax
import jax.numpy as jnp
from jax import lax
from jax.experimental import pallas as pl
from jax.experimental.pallas import tpu as pltpu
from jax.sharding import PartitionSpec as P

ITERS = 4
MESH = pl.DeviceIdType.MESH
THOLE = 0.39
F32 = jnp.float32
ROWS = 8


def lanes(index):
    return slice(index * 128, (index + 1) * 128)


def gathered(slot, rows_at, count, steps):
    blocks = []
    for start in range(0, slot.shape[0], 8):
        index = slot[start : start + 8]
        high = lax.shift_right_logical(index, 7)
        low = jnp.bitwise_and(index, 127)

        def pick(step, found):
            hit = high == step
            return tuple(
                jnp.where(
                    hit,
                    jnp.take_along_axis(jnp.broadcast_to(row, (8, 128)), low, axis=1),
                    old,
                )
                for row, old in zip(rows_at(step), found)
            )

        zero = jnp.zeros((8, 128), F32)
        blocks.append(lax.fori_loop(0, steps, pick, (zero,) * count, unroll=True))
    return blocks


def tiled_order_kernel(pos_ref, polar_ref, field_ref, atom_ref, pack_ref, inv_alpha_ref, rhs_ref, slot_ref):
    tiles = atom_ref.shape[0]
    atom = atom_ref[...]

    def rows_at(step):
        cols = pl.ds(pl.multiple_of(step * 128, 128), 128)
        rows = [pos_ref[c : c + 1, cols] for c in range(3)]
        rows += [field_ref[c : c + 1, cols] for c in range(3)]
        return rows + [polar_ref[pl.ds(step, 1), :]]

    for block, found in enumerate(gathered(atom, rows_at, 7, tiles)):
        for c in range(3):
            pack_ref[c * tiles + 8 * block : c * tiles + 8 * block + 8, :] = found[c]
            rhs_ref[c * tiles + 8 * block : c * tiles + 8 * block + 8, :] = found[3 + c]
        pack_ref[3 * tiles + 8 * block : 3 * tiles + 8 * block + 8, :] = lax.rsqrt(found[6])
        inv_alpha_ref[8 * block : 8 * block + 8, :] = 1.0 / found[6]

    high_ids = lax.broadcasted_iota(jnp.int32, (tiles, 128), 0)
    low_ids = lax.broadcasted_iota(jnp.int32, (128, 128), 0)
    lane_ids = lax.broadcasted_iota(jnp.int32, (tiles, 128), 1).astype(F32)
    high = lax.shift_right_logical(atom, 7)
    low = jnp.bitwise_and(atom, 127)
    total = None
    for pair in range(0, tiles, 2):
        left, right = [], []
        for step in (pair, pair + 1):
            hot = high_ids == high[step : step + 1]
            left.append(
                jnp.concatenate(
                    [jnp.where(hot, float(step), 0.0), jnp.where(hot, lane_ids, 0.0)], axis=0
                )
            )
            right.append(jnp.where(low_ids == low[step : step + 1], 1.0, 0.0))
        term = lax.dot_general(
            jnp.concatenate(left, axis=1).astype(jnp.bfloat16),
            jnp.concatenate(right, axis=1).astype(jnp.bfloat16),
            (((1,), (1,)), ((), ())),
            preferred_element_type=F32,
        )
        total = term if total is None else total + term
    slot_ref[...] = (total[:tiles] * 128.0 + total[tiles:]).astype(jnp.int32)


def atom_order_kernel(x_ref, r_ref, slot_ref, dipoles_ref, residual_ref):
    tiles = slot_ref.shape[0]

    def rows_at(step):
        return [ref[pl.ds(c * tiles + step, 1), :] for ref in (x_ref, r_ref) for c in range(3)]

    for block, found in enumerate(gathered(slot_ref[...], rows_at, 6, tiles)):
        for c in range(3):
            for h in range(8):
                dipoles_ref[c : c + 1, lanes(8 * block + h)] = found[c][h : h + 1, :]
                residual_ref[c : c + 1, lanes(8 * block + h)] = found[3 + c][h : h + 1, :]


def pair_tensor(left, right, diagonal):
    dx = right[0] - left[0]
    dy = right[1] - left[1]
    dz = right[2] - left[2]
    square = dx * dx + dy * dy + dz * dz
    if diagonal is not None:
        square = jnp.where(diagonal, 1.0, square)
    inv = lax.rsqrt(square)
    minus_u = square * (square * inv) * (left[3] * right[3])
    decay = jnp.exp(minus_u)
    inv_square = inv * inv
    inv_cube = inv * inv_square
    if diagonal is not None:
        inv_cube = jnp.where(diagonal, 0.0, inv_cube)
    rest = 1.0 - decay
    g3 = rest * inv_cube
    g5 = (rest + minus_u * decay) * inv_cube * (3.0 * inv_square)
    ax = g5 * dx
    ay = g5 * dy
    return (
        ax * dx - g3,
        ax * dy,
        ax * dz,
        ay * dy - g3,
        ay * dz,
        g5 * dz * dz - g3,
    )


def times(t, m):
    return (
        t[0] * m[0] + t[1] * m[1] + t[2] * m[2],
        t[1] * m[0] + t[3] * m[1] + t[4] * m[2],
        t[2] * m[0] + t[4] * m[1] + t[5] * m[2],
    )


def solve_kernel(
    group,
    inner,
    pack_ref,
    rhs_ref,
    inv_alpha_ref,
    list_ref,
    shift_ref,
    x_ref,
    r_ref,
    own_t,
    pair_t,
    part,
    cols_a,
    cols_b,
    win_p,
    win_0,
    win_1,
    win_2,
    win_3,
    top,
    ret_out,
    ret_in,
    right_rows,
    hot,
    colmat,
    gram,
    sums_1,
    sums_2,
    ring_send,
    ring_recv,
    sum_send,
    sum_recv,
):
    tiles = rhs_ref.shape[0] // 3
    me = lax.axis_index("gx")
    outer = group // inner
    row, col = me // inner, me % inner
    after = lax.rem(me + 1, group)
    before = lax.rem(me + group - 1, group)
    peers_1 = [row * inner + lax.rem(col + d, inner) for d in range(1, inner)]
    peers_2 = [lax.rem(row + d, outer) * inner + col for d in range(1, outer)]
    wins = (win_0, win_1, win_2, win_3)

    barrier = pltpu.get_barrier_semaphore()
    everyone = [after, before] + peers_1 + peers_2
    for peer in everyone:
        pl.semaphore_signal(barrier, inc=1, device_id={"gx": peer}, device_id_type=MESH)

    def ring_copy(src, dst, index, peer):
        return pltpu.make_async_remote_copy(
            src_ref=src,
            dst_ref=dst,
            send_sem=ring_send.at[index],
            recv_sem=ring_recv.at[index],
            device_id={"gx": peer},
            device_id_type=MESH,
        )

    def sum_copies(which, stage):
        buf = sums_1 if stage == 0 else sums_2
        at = col if stage == 0 else row
        peers = peers_1 if stage == 0 else peers_2
        base = which * (inner + outer) + stage * inner
        return [
            pltpu.make_async_remote_copy(
                src_ref=buf.at[which, at],
                dst_ref=buf.at[which, at],
                send_sem=sum_send.at[base + d],
                recv_sem=sum_recv.at[base + d],
                device_id={"gx": peer},
                device_id_type=MESH,
            )
            for d, peer in enumerate(peers)
        ]

    def sum_start(which, stage, value):
        buf = sums_1 if stage == 0 else sums_2
        buf[which, pl.ds(col if stage == 0 else row, 1)] = value[None]
        for copy in sum_copies(which, stage):
            copy.start()

    def sum_finish(which, stage):
        for copy in sum_copies(which, stage):
            copy.wait()
        buf = sums_1 if stage == 0 else sums_2
        total = buf[which, 0]
        for d in range(1, inner if stage == 0 else outer):
            total = total + buf[which, d]
        return total

    def inner_rows(a, b):
        return jnp.sum(a * b, axis=0, keepdims=True)

    sub_ids = lax.broadcasted_iota(jnp.int32, (16, 128), 0)
    lane_ids = lax.broadcasted_iota(jnp.int32, (16, 128), 1)

    def packed_sums(stack):
        totals = jnp.sum(stack, axis=1, keepdims=True)
        return jnp.sum(jnp.where(sub_ids == lane_ids, totals, 0.0), axis=0, keepdims=True)

    def unpacked(sums):
        gram[...] = jnp.broadcast_to(sums, (128, 128)).T

    rhs = rhs_ref[...]
    inv_alpha = inv_alpha_ref[...]
    inv_alpha_3 = jnp.concatenate([inv_alpha] * 3, axis=0)
    win_p[0 : 4 * tiles, :] = pack_ref[...]
    win_0[0 : 3 * tiles, :] = rhs
    colmat[...] = jnp.zeros((128, 128), F32)
    gram[...] = jnp.zeros((128, 128), F32)
    gram[0:1, :] = inner_rows(rhs, rhs)
    gram[1:2, :] = inner_rows(rhs, rhs * inv_alpha_3)

    steps = 128 // ROWS

    def spread(buf, ref, index, count):
        for c in range(count):
            line = ref[pl.ds(c * tiles + index, 1), :]
            buf[:, c] = jnp.broadcast_to(line, (128, 128)).T.reshape(steps, ROWS, 128)

    def right_lines(n, vector):
        first = n + jnp.where(n >= tiles, 3 * tiles, 0)
        lines = [win_p[pl.ds(first + c * tiles, 1), :] for c in range(4)]
        if vector is not None:
            lines = [lines[c] + vector[c] for c in range(3)] + lines[3:]
        lines[3] = lines[3] * (-THOLE)
        return [jnp.broadcast_to(line, (ROWS, 128)) for line in lines]

    block_sub = lax.broadcasted_iota(jnp.int32, (ROWS, 128), 0)
    block_lane = lax.broadcasted_iota(jnp.int32, (ROWS, 128), 1)

    def own_tensors(t, cols):
        right = right_lines(t, None)

        def block(i, carry):
            left = [cols[i, c] for c in range(4)]
            same = block_sub + i * ROWS == block_lane
            for k, value in enumerate(pair_tensor(left, right, same)):
                own_t[t, i, k] = value
            return carry

        lax.fori_loop(0, steps, block, 0, unroll=True)

    last = me == group - 1

    def pair_tensors(t, cols):
        for e in range(2):
            n = list_ref[t, e + 1]
            wrap = jnp.where(jnp.logical_and(n >= tiles, last), 4.0 * group, 0.0)
            vector = (
                wrap,
                shift_ref[0, t, e + 1].astype(F32) * 128.0,
                shift_ref[1, t, e + 1].astype(F32) * (2.0 * tiles),
            )
            right = right_lines(n, vector)

            def block(i, carry):
                left = [cols[i, c] for c in range(4)]
                for k, value in enumerate(pair_tensor(left, right, None)):
                    pair_t[t, e, i, k] = value
                return carry

            lax.fori_loop(0, steps, block, 0, unroll=True)

    def in_pairs(ref, count, work):
        spread(cols_a, ref, 0, count)

        def body(u, carry):
            t = 2 * u
            spread(cols_b, ref, t + 1, count)
            work(t, cols_a)
            spread(cols_a, ref, lax.rem(t + 2, tiles), count)
            work(t + 1, cols_b)
            return carry

        lax.fori_loop(0, tiles // 2, body, 0)

    def own_fields(win):
        def body(t, carry):
            m = [
                jnp.broadcast_to(win[pl.ds(c * tiles + t, 1), :], (ROWS, 128))
                for c in range(3)
            ]

            def block(i, inside):
                tensor = [own_t[t, i, k] for k in range(6)]
                for c, value in enumerate(times(tensor, m)):
                    part[t, i, c] = value
                return inside

            lax.fori_loop(0, steps, block, 0, unroll=True)
            return carry

        lax.fori_loop(0, tiles, body, 0)

    def right_fields(win):
        def work(t, cols):
            def block(i, sums):
                m = [cols[i, c] for c in range(3)]
                new = []
                for e in range(2):
                    tensor = [pair_t[t, e, i, k] for k in range(6)]
                    new += list(times(tensor, m))
                return tuple(a + b for a, b in zip(sums, new))

            sums = lax.fori_loop(0, steps, block, (jnp.zeros((ROWS, 128), F32),) * 6, unroll=True)
            for e in range(2):
                for c in range(3):
                    right_rows[pl.ds(2 * tiles * c + 2 * t + e, 1), :] = jnp.sum(
                        sums[3 * e + c], axis=0, keepdims=True
                    )

        in_pairs(win, 3, work)
        rows = right_rows[...]
        rows = jnp.concatenate(
            [rows[2 * tiles * c : 2 * tiles * (c + 1)] for c in range(3)], axis=1
        )
        first = rows.astype(jnp.bfloat16)
        rows = rows - first.astype(F32)
        second = rows.astype(jnp.bfloat16)
        third = (rows - second.astype(F32)).astype(jnp.bfloat16)
        split = jnp.concatenate([first, second, third], axis=0)
        total = jnp.dot(hot[...], split, preferred_element_type=F32)
        return [
            jnp.concatenate([half[:, lanes(c)] for c in range(3)], axis=0)
            for half in (total[0:tiles], total[tiles : 2 * tiles])
        ]

    full_lane = lax.broadcasted_iota(jnp.int32, (128, 128), 1)

    def gather_column(t):
        now = colmat[...]
        for c in range(3):
            total = jnp.sum(part[t, :, c].reshape(128, 128), axis=1, keepdims=True)
            now = jnp.where(full_lane == c * tiles + t, total, now)
        colmat[...] = now

    def left_fields(win):
        def one(t):
            gather_column(lax.rem(t + tiles - 1, tiles))
            m = []
            for e in range(2):
                n = list_ref[t, e + 1]
                first = n + jnp.where(n >= tiles, 2 * tiles, 0)
                m.append(
                    [
                        jnp.broadcast_to(win[pl.ds(first + c * tiles, 1), :], (ROWS, 128))
                        for c in range(3)
                    ]
                )

            def block(i, inside):
                sums = [part[t, i, c] for c in range(3)]
                for e in range(2):
                    tensor = [pair_t[t, e, i, k] for k in range(6)]
                    sums = [a + b for a, b in zip(sums, times(tensor, m[e]))]
                for c in range(3):
                    part[t, i, c] = sums[c]
                return inside

            lax.fori_loop(0, steps, block, 0, unroll=True)

        def body(u, carry):
            for step in range(4):
                one(4 * u + step)
            return carry

        lax.fori_loop(0, tiles // 4, body, 0)
        gather_column(tiles - 1)
        return colmat[...].T[0 : 3 * tiles]

    in_pairs(pack_ref, 4, own_tensors)

    pl.semaphore_wait(barrier, len(everyone))
    halo_p = ring_copy(pack_ref, win_p.at[4 * tiles : 8 * tiles], 0, before)
    halo_p.start()
    halos = [ring_copy(rhs_ref, win_0.at[3 * tiles : 6 * tiles], 1, before)]
    halos += [
        ring_copy(wins[k].at[0 : 3 * tiles], wins[k].at[3 * tiles : 6 * tiles], 1 + k, before)
        for k in range(1, ITERS)
    ]
    returns = [
        ring_copy(ret_out.at[k], ret_in.at[k], 1 + ITERS + k, after) for k in range(ITERS)
    ]
    halos[0].start()
    sum_start(0, 0, packed_sums(gram[0:16, :]))

    own_fields(win_0)

    hot_lane = lax.broadcasted_iota(jnp.int32, (1, 128), 1)

    def mark(t, carry):
        for e in range(2):
            value = jnp.where(hot_lane == list_ref[t, e + 1], 1.0, 0.0)
            gram[pl.ds(2 * t + e, 1), :] = value
        return carry

    lax.fori_loop(0, tiles, mark, 0)
    marks = gram[...].T[0 : 2 * tiles, 0 : 2 * tiles].astype(jnp.bfloat16)
    hot[...] = jnp.concatenate([marks] * 3, axis=1)
    gram[...] = jnp.zeros((128, 128), F32)

    sum_start(0, 1, sum_finish(0, 0))
    halo_p.wait()
    in_pairs(pack_ref, 4, pair_tensors)

    vectors = [rhs]
    pair_index = {}
    centre = None
    centre_row = None
    for k in range(ITERS):
        if k > 0:
            halos[k].start()
        kept, sent = right_fields(wins[k])
        ret_out[k] = sent
        if k > 0:
            own_fields(wins[k])
        returns[k].start()
        halos[k].wait()
        field = left_fields(wins[k])
        field = field + kept
        if k == 0:
            unpacked(sum_finish(0, 1))
            centre_row = gram[1:2, :] / gram[0:1, :]
            gram[...] = jnp.zeros((128, 128), F32)
            gram[0:1, :] = inner_rows(rhs, rhs)
            pair_index[(0, 0)] = 0
            shifted = jnp.concatenate([inv_alpha - centre_row] * 3, axis=0)
        returns[k].wait()
        now = vectors[k]
        new = shifted * now - (field + ret_in[k])
        if k + 1 < ITERS:
            wins[k + 1][0 : 3 * tiles, :] = new
        else:
            top[...] = new
        vectors = []
        for j in range(k + 2):
            if j == ITERS:
                vectors.append(top[...])
            else:
                vectors.append(rhs_ref[...] if j == 0 else wins[j][0 : 3 * tiles, :])
        for j in range(k + 2):
            pair_index[(j, k + 1)] = len(pair_index)
            index = pair_index[(j, k + 1)]
            gram[index : index + 1, :] = inner_rows(vectors[j], new)

    sum_start(1, 0, packed_sums(gram[0:16, :]))
    sum_start(1, 1, sum_finish(1, 0))
    unpacked(sum_finish(1, 1))

    def entry(a, b):
        index = pair_index[(min(a, b), max(a, b))]
        return gram[index : index + 1, :]

    def form(a, b):
        out = None
        for i, p in enumerate(a):
            for j, q in enumerate(b):
                term = p * q * entry(i, j)
                out = term if out is None else out + term
        return out

    def plus(a, scale, b):
        out = []
        for i in range(max(len(a), len(b))):
            term = scale * b[i] if i < len(b) else None
            if i < len(a):
                out.append(a[i] if term is None else a[i] + term)
            else:
                out.append(term)
        return out

    one = jnp.ones((1, 128), F32)
    x_coef = []
    r_coef = [one]
    d_coef = [one]
    norm_now = form(r_coef, r_coef)
    for iteration in range(ITERS):
        applied = [centre_row * v for v in d_coef] + [0.0 * one]
        applied = [
            applied[i] + d_coef[i - 1] if i > 0 else applied[i] for i in range(len(applied))
        ]
        step = norm_now / form(d_coef, applied)
        x_coef = plus(x_coef, step, d_coef)
        r_coef = plus(r_coef, -step, applied)
        if iteration + 1 < ITERS:
            norm_next = form(r_coef, r_coef)
            d_coef = plus(r_coef, norm_next / norm_now, d_coef)
            norm_now = norm_next

    for out_ref, coef in ((x_ref, x_coef), (r_ref, r_coef)):
        total = None
        for j, value in enumerate(coef):
            term = value * vectors[j]
            total = term if total is None else total + term
        out_ref[...] = total


def on_device(group, positions, polar, field_ext, tile_atom, tile_list, image_shift):
    atoms = tile_atom.shape[0]
    tiles = tile_list.shape[0]
    inner = 16 if group % 16 == 0 else 2
    outer = group // inner
    steps = 128 // ROWS
    vmem = pl.BlockSpec(memory_space=pltpu.VMEM)
    smem = pl.BlockSpec(memory_space=pltpu.SMEM)
    state = jax.ShapeDtypeStruct((3 * tiles, 128), F32)

    def shape(*dims, dtype=F32):
        return jax.ShapeDtypeStruct(dims, dtype)

    pack, inv_alpha, rhs, slot = pl.pallas_call(
        tiled_order_kernel,
        out_shape=(shape(4 * tiles, 128), shape(tiles, 128), state, shape(tiles, 128, dtype=jnp.int32)),
        in_specs=[vmem] * 4,
        out_specs=(vmem,) * 4,
        name="tiled_order",
    )(positions, polar.reshape(tiles, 128), field_ext, tile_atom.reshape(tiles, 128))

    sum_count = 2 * (inner + outer)
    ring_count = 1 + 2 * ITERS
    x, r = pl.pallas_call(
        functools.partial(solve_kernel, group, inner),
        out_shape=(state, state),
        in_specs=[vmem] * 3 + [smem] * 2,
        out_specs=(vmem,) * 2,
        scratch_shapes=[
            pltpu.VMEM((tiles, steps, 6, ROWS, 128), F32),
            pltpu.VMEM((tiles, 2, steps, 6, ROWS, 128), F32),
            pltpu.VMEM((tiles, steps, 3, ROWS, 128), F32),
            pltpu.VMEM((steps, 4, ROWS, 128), F32),
            pltpu.VMEM((steps, 4, ROWS, 128), F32),
            pltpu.VMEM((8 * tiles, 128), F32),
        ]
        + [pltpu.VMEM((6 * tiles, 128), F32)] * ITERS
        + [
            pltpu.VMEM((3 * tiles, 128), F32),
            pltpu.VMEM((ITERS, 3 * tiles, 128), F32),
            pltpu.VMEM((ITERS, 3 * tiles, 128), F32),
            pltpu.VMEM((6 * tiles, 128), F32),
            pltpu.VMEM((2 * tiles, 6 * tiles), jnp.bfloat16),
            pltpu.VMEM((128, 128), F32),
            pltpu.VMEM((128, 128), F32),
            pltpu.VMEM((2, inner, 1, 128), F32),
            pltpu.VMEM((2, outer, 1, 128), F32),
            pltpu.SemaphoreType.DMA((ring_count,)),
            pltpu.SemaphoreType.DMA((ring_count,)),
            pltpu.SemaphoreType.DMA((sum_count,)),
            pltpu.SemaphoreType.DMA((sum_count,)),
        ],
        compiler_params=pltpu.CompilerParams(
            collective_id=0, has_side_effects=True, vmem_limit_bytes=60 * 1024 * 1024
        ),
        name="solve",
    )(pack, rhs, inv_alpha, tile_list, image_shift)

    return pl.pallas_call(
        atom_order_kernel,
        out_shape=(shape(3, atoms), shape(3, atoms)),
        in_specs=[vmem] * 3,
        out_specs=(vmem,) * 2,
        name="atom_order",
    )(x, r, slot)


def solution(mesh):
    both = ("rep", "gx")
    return jax.shard_map(
        functools.partial(on_device, mesh.shape["gx"]),
        mesh=mesh,
        in_specs=(
            P(None, both),
            P(both),
            P(None, both),
            P(both),
            P(both, None),
            P(None, both, None),
        ),
        out_specs=(P(None, both), P(None, both)),
        check_vma=False,
    )
```

```python
import functools

import jax
import jax.numpy as jnp
from jax import lax
from jax.experimental import pallas as pl
from jax.experimental.pallas import tpu as pltpu
from jax.sharding import PartitionSpec as P

ITERS = 4
MESH = pl.DeviceIdType.MESH
THOLE = 0.39
F32 = jnp.float32
ROWS = 8


def lanes(index):
    return slice(index * 128, (index + 1) * 128)


def gathered(slot, rows_at, count, steps):
    blocks = []
    for start in range(0, slot.shape[0], 8):
        index = slot[start : start + 8]
        high = lax.shift_right_logical(index, 7)
        low = jnp.bitwise_and(index, 127)

        def pick(step, found):
            hit = high == step
            return tuple(
                jnp.where(
                    hit,
                    jnp.take_along_axis(jnp.broadcast_to(row, (8, 128)), low, axis=1),
                    old,
                )
                for row, old in zip(rows_at(step), found)
            )

        zero = jnp.zeros((8, 128), F32)
        blocks.append(lax.fori_loop(0, steps, pick, (zero,) * count, unroll=True))
    return blocks


def inverse_order(atom):
    tiles = atom.shape[0]
    high_ids = lax.broadcasted_iota(jnp.int32, (tiles, 128), 0)
    low_ids = lax.broadcasted_iota(jnp.int32, (128, 128), 0)
    lane_ids = lax.broadcasted_iota(jnp.int32, (tiles, 128), 1).astype(F32)
    high = lax.shift_right_logical(atom, 7)
    low = jnp.bitwise_and(atom, 127)
    total = None
    for pair in range(0, tiles, 2):
        left, right = [], []
        for step in (pair, pair + 1):
            hot = high_ids == high[step : step + 1]
            left.append(
                jnp.concatenate(
                    [jnp.where(hot, float(step), 0.0), jnp.where(hot, lane_ids, 0.0)], axis=0
                )
            )
            right.append(jnp.where(low_ids == low[step : step + 1], 1.0, 0.0))
        term = lax.dot_general(
            jnp.concatenate(left, axis=1).astype(jnp.bfloat16),
            jnp.concatenate(right, axis=1).astype(jnp.bfloat16),
            (((1,), (1,)), ((), ())),
            preferred_element_type=F32,
        )
        total = term if total is None else total + term
    return (total[:tiles] * 128.0 + total[tiles:]).astype(jnp.int32)


def atom_order_kernel(x_ref, r_ref, slot_ref, dipoles_ref, residual_ref):
    tiles = slot_ref.shape[0]

    def rows_at(step):
        return [ref[pl.ds(c * tiles + step, 1), :] for ref in (x_ref, r_ref) for c in range(3)]

    for block, found in enumerate(gathered(slot_ref[...], rows_at, 6, tiles)):
        for c in range(3):
            for h in range(8):
                dipoles_ref[c : c + 1, lanes(8 * block + h)] = found[c][h : h + 1, :]
                residual_ref[c : c + 1, lanes(8 * block + h)] = found[3 + c][h : h + 1, :]


def pair_tensor(left, right, diagonal):
    dx = right[0] - left[0]
    dy = right[1] - left[1]
    dz = right[2] - left[2]
    square = dx * dx + dy * dy + dz * dz
    if diagonal is not None:
        square = jnp.where(diagonal, 1.0, square)
    inv = lax.rsqrt(square)
    minus_u = square * (square * inv) * (left[3] * right[3])
    decay = jnp.exp(minus_u)
    inv_square = inv * inv
    inv_cube = inv * inv_square
    if diagonal is not None:
        inv_cube = jnp.where(diagonal, 0.0, inv_cube)
    rest = 1.0 - decay
    g3 = rest * inv_cube
    g5 = (rest + minus_u * decay) * inv_cube * (3.0 * inv_square)
    ax = g5 * dx
    ay = g5 * dy
    return (
        ax * dx - g3,
        ax * dy,
        ax * dz,
        ay * dy - g3,
        ay * dz,
        g5 * dz * dz - g3,
    )


def times(t, m):
    return (
        t[0] * m[0] + t[1] * m[1] + t[2] * m[2],
        t[1] * m[0] + t[3] * m[1] + t[4] * m[2],
        t[2] * m[0] + t[4] * m[1] + t[5] * m[2],
    )


def solve_kernel(
    group,
    inner,
    pos_ref,
    polar_ref,
    field_ref,
    atom_ref,
    list_ref,
    shift_ref,
    x_ref,
    r_ref,
    slot_ref,
    inv_alpha_ref,
    own_t,
    pair_t,
    part,
    cols_a,
    cols_b,
    win_p,
    win_0,
    win_1,
    win_2,
    win_3,
    top,
    ret_out,
    ret_in,
    right_rows,
    own_rows,
    hot,
    colmat,
    gram,
    sums_1,
    sums_2,
    ring_send,
    ring_recv,
    sum_send,
    sum_recv,
):
    tiles = atom_ref.shape[0]
    me = lax.axis_index("gx")
    outer = group // inner
    row, col = me // inner, me % inner
    after = lax.rem(me + 1, group)
    before = lax.rem(me + group - 1, group)
    peers_1 = [row * inner + lax.rem(col + d, inner) for d in range(1, inner)]
    peers_2 = [lax.rem(row + d, outer) * inner + col for d in range(1, outer)]
    wins = (win_0, win_1, win_2, win_3)

    barrier = pltpu.get_barrier_semaphore()
    everyone = [after, before] + peers_1 + peers_2
    for peer in everyone:
        pl.semaphore_signal(barrier, inc=1, device_id={"gx": peer}, device_id_type=MESH)

    def ring_copy(src, dst, index, peer):
        return pltpu.make_async_remote_copy(
            src_ref=src,
            dst_ref=dst,
            send_sem=ring_send.at[index],
            recv_sem=ring_recv.at[index],
            device_id={"gx": peer},
            device_id_type=MESH,
        )

    def sum_copies(which, stage):
        buf = sums_1 if stage == 0 else sums_2
        at = col if stage == 0 else row
        peers = peers_1 if stage == 0 else peers_2
        base = which * (inner + outer) + stage * inner
        return [
            pltpu.make_async_remote_copy(
                src_ref=buf.at[which, at],
                dst_ref=buf.at[which, at],
                send_sem=sum_send.at[base + d],
                recv_sem=sum_recv.at[base + d],
                device_id={"gx": peer},
                device_id_type=MESH,
            )
            for d, peer in enumerate(peers)
        ]

    def sum_start(which, stage, value):
        buf = sums_1 if stage == 0 else sums_2
        buf[which, pl.ds(col if stage == 0 else row, 1)] = value[None]
        for copy in sum_copies(which, stage):
            copy.start()

    def sum_finish(which, stage):
        for copy in sum_copies(which, stage):
            copy.wait()
        buf = sums_1 if stage == 0 else sums_2
        total = buf[which, 0]
        for d in range(1, inner if stage == 0 else outer):
            total = total + buf[which, d]
        return total

    def inner_rows(a, b):
        return jnp.sum(a * b, axis=0, keepdims=True)

    sub_ids = lax.broadcasted_iota(jnp.int32, (16, 128), 0)
    lane_ids = lax.broadcasted_iota(jnp.int32, (16, 128), 1)

    def packed_sums(stack):
        totals = jnp.sum(stack, axis=1, keepdims=True)
        return jnp.sum(jnp.where(sub_ids == lane_ids, totals, 0.0), axis=0, keepdims=True)

    def unpacked(sums):
        gram[...] = jnp.broadcast_to(sums, (128, 128)).T

    def rows_at(step):
        places = pl.ds(pl.multiple_of(step * 128, 128), 128)
        rows = [pos_ref[c : c + 1, places] for c in range(3)]
        rows += [field_ref[c : c + 1, places] for c in range(3)]
        return rows + [polar_ref[pl.ds(step, 1), :]]

    for block, found in enumerate(gathered(atom_ref[...], rows_at, 7, tiles)):
        for c in range(3):
            at = c * tiles + 8 * block
            win_p[at : at + 8, :] = found[c]
            win_0[at : at + 8, :] = found[3 + c]
        at = 3 * tiles + 8 * block
        win_p[at : at + 8, :] = lax.rsqrt(found[6])
        inv_alpha_ref[8 * block : 8 * block + 8, :] = 1.0 / found[6]

    rhs = win_0[0 : 3 * tiles, :]
    inv_alpha = inv_alpha_ref[...]
    inv_alpha_3 = jnp.concatenate([inv_alpha] * 3, axis=0)
    colmat[...] = jnp.zeros((128, 128), F32)
    gram[...] = jnp.zeros((128, 128), F32)
    gram[0:1, :] = inner_rows(rhs, rhs)
    gram[1:2, :] = inner_rows(rhs, rhs * inv_alpha_3)

    steps = 128 // ROWS

    def spread(buf, ref, index, count):
        for c in range(count):
            line = ref[pl.ds(c * tiles + index, 1), :]
            buf[:, c] = jnp.broadcast_to(line, (128, 128)).T.reshape(steps, ROWS, 128)

    def right_lines(n, vector):
        first = n + jnp.where(n >= tiles, 3 * tiles, 0)
        lines = [win_p[pl.ds(first + c * tiles, 1), :] for c in range(4)]
        if vector is not None:
            lines = [lines[c] + vector[c] for c in range(3)] + lines[3:]
        lines[3] = lines[3] * (-THOLE)
        return [jnp.broadcast_to(line, (ROWS, 128)) for line in lines]

    block_sub = lax.broadcasted_iota(jnp.int32, (ROWS, 128), 0)
    block_lane = lax.broadcasted_iota(jnp.int32, (ROWS, 128), 1)

    def own_tensors(t, cols):
        right = right_lines(t, None)

        def block(i, carry):
            left = [cols[i, c] for c in range(4)]
            same = block_sub + i * ROWS == block_lane
            for k, value in enumerate(pair_tensor(left, right, same)):
                own_t[t, i, k] = value
            return carry

        lax.fori_loop(0, steps, block, 0, unroll=True)

    last = me == group - 1

    def pair_tensors(t, cols):
        for e in range(2):
            n = list_ref[e + 1, t]
            wrap = jnp.where(jnp.logical_and(n >= tiles, last), 4.0 * group, 0.0)
            vector = (
                wrap,
                shift_ref[e + 1, 0, t].astype(F32) * 128.0,
                shift_ref[e + 1, 1, t].astype(F32) * (2.0 * tiles),
            )
            right = right_lines(n, vector)

            def block(i, carry):
                left = [cols[i, c] for c in range(4)]
                for k, value in enumerate(pair_tensor(left, right, None)):
                    pair_t[t, e, i, k] = value
                return carry

            lax.fori_loop(0, steps, block, 0, unroll=True)

    def in_pairs(ref, count, work, first=0, stop=tiles):
        spread(cols_a, ref, first, count)

        def body(u, carry):
            t = first + 2 * u
            spread(cols_b, ref, t + 1, count)
            work(t, cols_a)
            spread(cols_a, ref, lax.rem(t + 2, tiles), count)
            work(t + 1, cols_b)
            return carry

        lax.fori_loop(0, (stop - first) // 2, body, 0)

    def own_fields(win, first=0, stop=tiles):
        def body(t, carry):
            m = [
                jnp.broadcast_to(win[pl.ds(c * tiles + t, 1), :], (ROWS, 128))
                for c in range(3)
            ]

            def block(i, inside):
                tensor = [own_t[t, i, k] for k in range(6)]
                for c, value in enumerate(times(tensor, m)):
                    part[t, i, c] = value
                return inside

            lax.fori_loop(0, steps, block, 0, unroll=True)
            return carry

        lax.fori_loop(first, stop, body, 0)

    def right_fields(win, with_own):
        sources = 3 if with_own else 2

        def work(t, cols):
            def block(i, sums):
                m = [cols[i, c] for c in range(3)]
                new = []
                for e in range(sources):
                    tensor = [own_t[t, i, k] if e == 2 else pair_t[t, e, i, k] for k in range(6)]
                    new += list(times(tensor, m))
                return tuple(a + b for a, b in zip(sums, new))

            zeros = (jnp.zeros((ROWS, 128), F32),) * (3 * sources)
            sums = lax.fori_loop(0, steps, block, zeros, unroll=True)
            if with_own:
                for c in range(3):
                    own_rows[pl.ds(c * tiles + t, 1), :] = jnp.sum(
                        sums[6 + c], axis=0, keepdims=True
                    )
            for e in range(2):
                for c in range(3):
                    right_rows[pl.ds(2 * tiles * c + 2 * t + e, 1), :] = jnp.sum(
                        sums[3 * e + c], axis=0, keepdims=True
                    )

        in_pairs(win, 3, work)
        rows = right_rows[...]
        rows = jnp.concatenate(
            [rows[2 * tiles * c : 2 * tiles * (c + 1)] for c in range(3)], axis=1
        )
        first = rows.astype(jnp.bfloat16)
        rows = rows - first.astype(F32)
        second = rows.astype(jnp.bfloat16)
        third = (rows - second.astype(F32)).astype(jnp.bfloat16)
        split = jnp.concatenate([first, second, third], axis=0)
        total = jnp.dot(hot[...], split, preferred_element_type=F32)
        return [
            jnp.concatenate([half[:, lanes(c)] for c in range(3)], axis=0)
            for half in (total[0:tiles], total[tiles : 2 * tiles])
        ]

    full_lane = lax.broadcasted_iota(jnp.int32, (128, 128), 1)

    def gather_column(t):
        now = colmat[...]
        for c in range(3):
            total = jnp.sum(part[t, :, c].reshape(128, 128), axis=1, keepdims=True)
            now = jnp.where(full_lane == c * tiles + t, total, now)
        colmat[...] = now

    def left_fields(win, with_part):
        def one(t):
            gather_column(lax.rem(t + tiles - 1, tiles))
            m = []
            for e in range(2):
                n = list_ref[e + 1, t]
                first = n + jnp.where(n >= tiles, 2 * tiles, 0)
                m.append(
                    [
                        jnp.broadcast_to(win[pl.ds(first + c * tiles, 1), :], (ROWS, 128))
                        for c in range(3)
                    ]
                )

            def block(i, inside):
                sums = [part[t, i, c] for c in range(3)] if with_part else None
                for e in range(2):
                    tensor = [pair_t[t, e, i, k] for k in range(6)]
                    new = times(tensor, m[e])
                    sums = new if sums is None else [a + b for a, b in zip(sums, new)]
                for c in range(3):
                    part[t, i, c] = sums[c]
                return inside

            lax.fori_loop(0, steps, block, 0, unroll=True)

        def body(u, carry):
            for step in range(4):
                one(4 * u + step)
            return carry

        lax.fori_loop(0, tiles // 4, body, 0)
        gather_column(tiles - 1)
        return colmat[...].T[0 : 3 * tiles]

    in_pairs(win_p, 4, own_tensors, 0, tiles // 2)

    pl.semaphore_wait(barrier, len(everyone))
    own_p, own_v = 4 * tiles, 3 * tiles
    halo_p = ring_copy(win_p.at[0:own_p], win_p.at[own_p : 2 * own_p], 0, before)
    halo_p.start()
    halos = [
        ring_copy(win.at[0:own_v], win.at[own_v : 2 * own_v], 1 + k, before)
        for k, win in enumerate(wins)
    ]
    returns = [
        ring_copy(ret_out.at[k], ret_in.at[k], 1 + ITERS + k, after) for k in range(ITERS)
    ]
    halos[0].start()
    sum_start(0, 0, packed_sums(gram[0:16, :]))

    in_pairs(win_p, 4, own_tensors, tiles // 2, tiles)
    own_fields(win_0)

    hot_lane = lax.broadcasted_iota(jnp.int32, (1, 128), 1)

    def mark(t, carry):
        for e in range(2):
            value = jnp.where(hot_lane == list_ref[e + 1, t], 1.0, 0.0)
            gram[pl.ds(2 * t + e, 1), :] = value
        return carry

    lax.fori_loop(0, tiles, mark, 0)
    marks = gram[...].T[0 : 2 * tiles, 0 : 2 * tiles].astype(jnp.bfloat16)
    hot[...] = jnp.concatenate([marks] * 3, axis=1)
    gram[...] = jnp.zeros((128, 128), F32)
    slot_ref[...] = inverse_order(atom_ref[...])

    halo_p.wait()
    in_pairs(win_p, 4, pair_tensors)
    sum_start(0, 1, sum_finish(0, 0))

    def own_vector(k):
        return wins[k][0:own_v, :]

    pair_index = {}

    def keep(key, line):
        index = pair_index[key] = len(pair_index)
        gram[index : index + 1, :] = line

    centre = None
    for k in range(ITERS):
        final = k + 1 == ITERS
        if k > 0:
            for j in range(k + 1):
                keep((j, k), inner_rows(own_vector(j), own_vector(k)))
            halos[k].start()
        kept, sent = right_fields(wins[k], final)
        ret_out[k] = sent
        if k > 0 and not final:
            own_fields(wins[k], 0, 4)
        if final:
            now = own_vector(k)
            line = inner_rows(now, shifted * now - (own_rows[...] + 2.0 * kept))
            kept = kept + own_rows[...]
        returns[k].start()
        if k > 0 and not final:
            own_fields(wins[k], 4, tiles)
        halos[k].wait()
        if final:
            line = line - 2.0 * inner_rows(wins[k][own_v : 2 * own_v, :], sent)
            keep((k, k + 1), line)
            sum_start(1, 0, packed_sums(gram[0:16, :]))
        field = left_fields(wins[k], not final) + kept
        if k == 0:
            unpacked(sum_finish(0, 1))
            centre = gram[1:2, :] / gram[0:1, :]
            gram[...] = jnp.zeros((128, 128), F32)
            keep((0, 0), inner_rows(rhs, rhs))
            shifted = jnp.concatenate([inv_alpha - centre] * 3, axis=0)
        if final:
            sum_start(1, 1, sum_finish(1, 0))
        returns[k].wait()
        new = shifted * own_vector(k) - (field + ret_in[k])
        if final:
            top[...] = new
        else:
            wins[k + 1][0:own_v, :] = new

    unpacked(sum_finish(1, 1))
    vectors = [own_vector(k) for k in range(ITERS)] + [top[...]]
    for j in range(ITERS - 1):
        pair_index[(j, ITERS)] = pair_index[(j + 1, ITERS - 1)]

    def entry(a, b):
        index = pair_index[(min(a, b), max(a, b))]
        return gram[index : index + 1, :]

    def form(a, b):
        out = None
        for i, p in enumerate(a):
            for j, q in enumerate(b):
                term = p * q * entry(i, j)
                out = term if out is None else out + term
        return out

    def plus(a, scale, b):
        out = []
        for i in range(max(len(a), len(b))):
            term = scale * b[i] if i < len(b) else None
            if i < len(a):
                out.append(a[i] if term is None else a[i] + term)
            else:
                out.append(term)
        return out

    one = jnp.ones((1, 128), F32)
    x_coef = []
    r_coef = [one]
    d_coef = [one]
    norm_now = form(r_coef, r_coef)
    for iteration in range(ITERS):
        applied = [centre * v for v in d_coef] + [0.0 * one]
        applied = [
            applied[i] + d_coef[i - 1] if i > 0 else applied[i] for i in range(len(applied))
        ]
        step = norm_now / form(d_coef, applied)
        x_coef = plus(x_coef, step, d_coef)
        r_coef = plus(r_coef, -step, applied)
        if iteration + 1 < ITERS:
            norm_next = form(r_coef, r_coef)
            d_coef = plus(r_coef, norm_next / norm_now, d_coef)
            norm_now = norm_next

    for out_ref, coef in ((x_ref, x_coef), (r_ref, r_coef)):
        total = None
        for j, value in enumerate(coef):
            term = value * vectors[j]
            total = term if total is None else total + term
        out_ref[...] = total


def on_device(group, positions, polar, field_ext, tile_atom, tile_list, image_shift):
    atoms = tile_atom.shape[0]
    tiles = tile_list.shape[0]
    inner = 16 if group % 16 == 0 else 2
    outer = group // inner
    steps = 128 // ROWS
    vmem = pl.BlockSpec(memory_space=pltpu.VMEM)
    smem = pl.BlockSpec(memory_space=pltpu.SMEM)
    state = jax.ShapeDtypeStruct((3 * tiles, 128), F32)

    def shape(*dims, dtype=F32):
        return jax.ShapeDtypeStruct(dims, dtype)

    sum_count = 2 * (inner + outer)
    ring_count = 1 + 2 * ITERS
    x, r, slot = pl.pallas_call(
        functools.partial(solve_kernel, group, inner),
        out_shape=(state, state, shape(tiles, 128, dtype=jnp.int32)),
        in_specs=[vmem] * 4 + [smem] * 2,
        out_specs=(vmem,) * 3,
        scratch_shapes=[
            pltpu.VMEM((tiles, 128), F32),
            pltpu.VMEM((tiles, steps, 6, ROWS, 128), F32),
            pltpu.VMEM((tiles, 2, steps, 6, ROWS, 128), F32),
            pltpu.VMEM((tiles, steps, 3, ROWS, 128), F32),
            pltpu.VMEM((steps, 4, ROWS, 128), F32),
            pltpu.VMEM((steps, 4, ROWS, 128), F32),
            pltpu.VMEM((8 * tiles, 128), F32),
        ]
        + [pltpu.VMEM((6 * tiles, 128), F32)] * ITERS
        + [
            pltpu.VMEM((3 * tiles, 128), F32),
            pltpu.VMEM((ITERS, 3 * tiles, 128), F32),
            pltpu.VMEM((ITERS, 3 * tiles, 128), F32),
            pltpu.VMEM((6 * tiles, 128), F32),
            pltpu.VMEM((3 * tiles, 128), F32),
            pltpu.VMEM((2 * tiles, 6 * tiles), jnp.bfloat16),
            pltpu.VMEM((128, 128), F32),
            pltpu.VMEM((128, 128), F32),
            pltpu.VMEM((2, inner, 1, 128), F32),
            pltpu.VMEM((2, outer, 1, 128), F32),
            pltpu.SemaphoreType.DMA((ring_count,)),
            pltpu.SemaphoreType.DMA((ring_count,)),
            pltpu.SemaphoreType.DMA((sum_count,)),
            pltpu.SemaphoreType.DMA((sum_count,)),
        ],
        compiler_params=pltpu.CompilerParams(
            collective_id=0, has_side_effects=True, vmem_limit_bytes=60 * 1024 * 1024
        ),
        name="solve",
    )(
        positions,
        polar.reshape(tiles, 128),
        field_ext,
        tile_atom.reshape(tiles, 128),
        tile_list.T,
        image_shift.transpose(2, 0, 1),
    )

    return pl.pallas_call(
        atom_order_kernel,
        out_shape=(shape(3, atoms), shape(3, atoms)),
        in_specs=[vmem] * 3,
        out_specs=(vmem,) * 2,
        name="atom_order",
    )(x, r, slot)


def solution(mesh):
    both = ("rep", "gx")
    return jax.shard_map(
        functools.partial(on_device, mesh.shape["gx"]),
        mesh=mesh,
        in_specs=(
            P(None, both),
            P(both),
            P(None, both),
            P(both),
            P(both, None),
            P(None, both, None),
        ),
        out_specs=(P(None, both), P(None, both)),
        check_vma=False,
    )
```

```python
import functools
import math

import jax
import jax.numpy as jnp
from jax import lax
from jax.experimental import pallas as pl
from jax.experimental.pallas import tpu as pltpu
from jax.sharding import PartitionSpec as P

ITERS = 4
MESH = pl.DeviceIdType.MESH
THOLE = 0.39
F32 = jnp.float32
ROWS = 8


def lanes(index):
    return slice(index * 128, (index + 1) * 128)


def gathered(slot, rows_at, count, steps):
    blocks = []
    for start in range(0, slot.shape[0], 8):
        index = slot[start : start + 8]
        high = lax.shift_right_logical(index, 7)
        low = jnp.bitwise_and(index, 127)

        def pick(step, found):
            hit = high == step
            return tuple(
                jnp.where(
                    hit,
                    jnp.take_along_axis(jnp.broadcast_to(row, (8, 128)), low, axis=1),
                    old,
                )
                for row, old in zip(rows_at(step), found)
            )

        zero = jnp.zeros((8, 128), F32)
        blocks.append(lax.fori_loop(0, steps, pick, (zero,) * count, unroll=True))
    return blocks


def inverse_order(atom):
    tiles = atom.shape[0]
    high_ids = lax.broadcasted_iota(jnp.int32, (tiles, 128), 0)
    low_ids = lax.broadcasted_iota(jnp.int32, (128, 128), 0)
    lane_ids = lax.broadcasted_iota(jnp.int32, (tiles, 128), 1).astype(F32)
    high = lax.shift_right_logical(atom, 7)
    low = jnp.bitwise_and(atom, 127)
    total = None
    for pair in range(0, tiles, 2):
        left, right = [], []
        for step in (pair, pair + 1):
            hot = high_ids == high[step : step + 1]
            left.append(
                jnp.concatenate(
                    [jnp.where(hot, float(step), 0.0), jnp.where(hot, lane_ids, 0.0)], axis=0
                )
            )
            right.append(jnp.where(low_ids == low[step : step + 1], 1.0, 0.0))
        term = lax.dot_general(
            jnp.concatenate(left, axis=1).astype(jnp.bfloat16),
            jnp.concatenate(right, axis=1).astype(jnp.bfloat16),
            (((1,), (1,)), ((), ())),
            preferred_element_type=F32,
        )
        total = term if total is None else total + term
    return (total[:tiles] * 128.0 + total[tiles:]).astype(jnp.int32)


def atom_order_kernel(x_ref, r_ref, slot_ref, dipoles_ref, residual_ref):
    tiles = slot_ref.shape[0]

    def rows_at(step):
        return [ref[pl.ds(c * tiles + step, 1), :] for ref in (x_ref, r_ref) for c in range(3)]

    for block, found in enumerate(gathered(slot_ref[...], rows_at, 6, tiles)):
        for c in range(3):
            for h in range(8):
                dipoles_ref[c : c + 1, lanes(8 * block + h)] = found[c][h : h + 1, :]
                residual_ref[c : c + 1, lanes(8 * block + h)] = found[3 + c][h : h + 1, :]


def pair_tensor(left, right, diagonal):
    dx = right[0] - left[0]
    dy = right[1] - left[1]
    dz = right[2] - left[2]
    square = dx * dx + dy * dy + dz * dz
    if diagonal is not None:
        square = jnp.where(diagonal, 1.0, square)
    inv = lax.rsqrt(square)
    minus_u = square * (square * inv) * (left[3] * right[3])
    decay = jnp.exp(minus_u)
    inv_cube = inv * (inv * inv)
    rest = 1.0 - decay
    g3 = rest * inv_cube
    if diagonal is not None:
        g3 = jnp.where(diagonal, 0.0, g3)
    damped = (rest + minus_u * decay) * inv_cube
    scale = (damped * lax.rsqrt(damped)) * (inv * math.sqrt(3.0))
    return (dx * scale, dy * scale, dz * scale), g3


def along(e, m):
    share = e[0] * m[0] + e[1] * m[1] + e[2] * m[2]
    return (e[0] * share, e[1] * share, e[2] * share)


def solve_kernel(
    group,
    inner,
    pos_ref,
    polar_ref,
    field_ref,
    atom_ref,
    list_ref,
    shift_ref,
    x_ref,
    r_ref,
    slot_ref,
    inv_alpha_ref,
    own_t,
    pair_t,
    part,
    cols_a,
    cols_b,
    win_p,
    win_0,
    win_1,
    win_2,
    win_3,
    top,
    ret_out,
    ret_in,
    right_rows,
    own_rows,
    left_rows,
    scalar_t,
    hot,
    colmat,
    gram,
    sums_1,
    sums_2,
    ring_send,
    ring_recv,
    sum_send,
    sum_recv,
):
    tiles = atom_ref.shape[0]
    me = lax.axis_index("gx")
    outer = group // inner
    row, col = me // inner, me % inner
    after = lax.rem(me + 1, group)
    before = lax.rem(me + group - 1, group)
    peers_1 = [row * inner + lax.rem(col + d, inner) for d in range(1, inner)]
    peers_2 = [lax.rem(row + d, outer) * inner + col for d in range(1, outer)]
    wins = (win_0, win_1, win_2, win_3)

    barrier = pltpu.get_barrier_semaphore()
    everyone = [after, before] + peers_1 + peers_2
    for peer in everyone:
        pl.semaphore_signal(barrier, inc=1, device_id={"gx": peer}, device_id_type=MESH)

    def ring_copy(src, dst, index, peer):
        return pltpu.make_async_remote_copy(
            src_ref=src,
            dst_ref=dst,
            send_sem=ring_send.at[index],
            recv_sem=ring_recv.at[index],
            device_id={"gx": peer},
            device_id_type=MESH,
        )

    def sum_copies(which, stage):
        buf = sums_1 if stage == 0 else sums_2
        at = col if stage == 0 else row
        peers = peers_1 if stage == 0 else peers_2
        base = which * (inner + outer) + stage * inner
        return [
            pltpu.make_async_remote_copy(
                src_ref=buf.at[which, at],
                dst_ref=buf.at[which, at],
                send_sem=sum_send.at[base + d],
                recv_sem=sum_recv.at[base + d],
                device_id={"gx": peer},
                device_id_type=MESH,
            )
            for d, peer in enumerate(peers)
        ]

    def sum_start(which, stage, value):
        buf = sums_1 if stage == 0 else sums_2
        buf[which, pl.ds(col if stage == 0 else row, 1)] = value[None]
        for copy in sum_copies(which, stage):
            copy.start()

    def sum_finish(which, stage):
        for copy in sum_copies(which, stage):
            copy.wait()
        buf = sums_1 if stage == 0 else sums_2
        total = buf[which, 0]
        for d in range(1, inner if stage == 0 else outer):
            total = total + buf[which, d]
        return total

    def inner_rows(a, b):
        return jnp.sum(a * b, axis=0, keepdims=True)

    sub_ids = lax.broadcasted_iota(jnp.int32, (16, 128), 0)
    lane_ids = lax.broadcasted_iota(jnp.int32, (16, 128), 1)

    def packed_sums(stack):
        totals = jnp.sum(stack, axis=1, keepdims=True)
        return jnp.sum(jnp.where(sub_ids == lane_ids, totals, 0.0), axis=0, keepdims=True)

    def unpacked(sums):
        gram[...] = jnp.broadcast_to(sums, (128, 128)).T

    def rows_at(step):
        places = pl.ds(pl.multiple_of(step * 128, 128), 128)
        rows = [pos_ref[c : c + 1, places] for c in range(3)]
        rows += [field_ref[c : c + 1, places] for c in range(3)]
        return rows + [polar_ref[pl.ds(step, 1), :]]

    for block, found in enumerate(gathered(atom_ref[...], rows_at, 7, tiles)):
        for c in range(3):
            at = c * tiles + 8 * block
            win_p[at : at + 8, :] = found[c]
            win_0[at : at + 8, :] = found[3 + c]
        at = 3 * tiles + 8 * block
        win_p[at : at + 8, :] = lax.rsqrt(found[6])
        inv_alpha_ref[8 * block : 8 * block + 8, :] = 1.0 / found[6]

    rhs = win_0[0 : 3 * tiles, :]
    inv_alpha = inv_alpha_ref[...]
    inv_alpha_3 = jnp.concatenate([inv_alpha] * 3, axis=0)
    colmat[...] = jnp.zeros((128, 128), F32)
    gram[...] = jnp.zeros((128, 128), F32)
    gram[0:1, :] = inner_rows(rhs, rhs)
    gram[1:2, :] = inner_rows(rhs, rhs * inv_alpha_3)

    steps = 128 // ROWS

    def spread(buf, ref, index, count):
        for c in range(count):
            line = ref[pl.ds(c * tiles + index, 1), :]
            buf[:, c] = jnp.broadcast_to(line, (128, 128)).T.reshape(steps, ROWS, 128)

    def right_lines(n, vector):
        first = n + jnp.where(n >= tiles, 3 * tiles, 0)
        lines = [win_p[pl.ds(first + c * tiles, 1), :] for c in range(4)]
        if vector is not None:
            lines = [lines[c] + vector[c] for c in range(3)] + lines[3:]
        lines[3] = lines[3] * (-THOLE)
        return [jnp.broadcast_to(line, (2 * ROWS, 128)) for line in lines]

    sub_16 = lax.broadcasted_iota(jnp.int32, (2 * ROWS, 128), 0)
    lane_16 = lax.broadcasted_iota(jnp.int32, (2 * ROWS, 128), 1)
    sub_8 = lax.broadcasted_iota(jnp.int32, (ROWS, 128), 0)
    lines_of = [jnp.logical_or(sub_8 == c, sub_8 == c + 3) for c in range(3)]
    halves = [jnp.logical_or(sub_16 == c, sub_16 == c + 3) for c in range(3)]

    def tensors(t, cols, right, diagonal, where, place):
        def block(i, carry):
            left = [cols[pl.ds(2 * i, 2), c].reshape(2 * ROWS, 128) for c in range(4)]
            same = sub_16 + i * (2 * ROWS) == lane_16 if diagonal else None
            e, g3 = pair_tensor(left, right, same)
            for c in range(3):
                where(t, i, c, e[c].reshape(2, ROWS, 128))
            high = g3.astype(jnp.bfloat16)
            low = (g3 - high.astype(F32)).astype(jnp.bfloat16)
            at = pl.multiple_of(i * (2 * ROWS), 2 * ROWS)
            scalar_t[t, pl.ds(at, 2 * ROWS), lanes(place)] = high
            scalar_t[t, pl.ds(128 + at, 2 * ROWS), lanes(place)] = low
            return carry

        lax.fori_loop(0, steps // 2, block, 0, unroll=True)

    def own_tensors(t, cols):
        def where(t, i, c, value):
            own_t[t, pl.ds(2 * i, 2), c] = value

        tensors(t, cols, right_lines(t, None), True, where, 2)

    def split_lines(lines):
        wide = jnp.where(halves[0], lines[0], jnp.where(halves[1], lines[1], lines[2]))
        high = wide.astype(jnp.bfloat16).astype(F32)
        return jnp.where(sub_16 < 3, high, wide - high).astype(jnp.bfloat16)

    last = me == group - 1

    def pair_tensors(t, cols):
        for e in range(2):
            n = list_ref[e + 1, t]
            wrap = jnp.where(jnp.logical_and(n >= tiles, last), 4.0 * group, 0.0)
            vector = (
                wrap,
                shift_ref[e + 1, 0, t].astype(F32) * 128.0,
                shift_ref[e + 1, 1, t].astype(F32) * (2.0 * tiles),
            )

            def where(t, i, c, value, e=e):
                pair_t[t, e, pl.ds(2 * i, 2), c] = value

            tensors(t, cols, right_lines(n, vector), False, where, e)

    def in_pairs(ref, count, work, first=0, stop=tiles):
        spread(cols_a, ref, first, count)

        def body(u, carry):
            t = first + 2 * u
            spread(cols_b, ref, t + 1, count)
            work(t, cols_a)
            spread(cols_a, ref, lax.rem(t + 2, tiles), count)
            work(t + 1, cols_b)
            return carry

        lax.fori_loop(0, (stop - first) // 2, body, 0)

    def own_fields(win, first=0, stop=tiles):
        def body(t, carry):
            m = [
                jnp.broadcast_to(win[pl.ds(c * tiles + t, 1), :], (ROWS, 128))
                for c in range(3)
            ]

            def block(i, inside):
                tensor = [own_t[t, i, c] for c in range(3)]
                for c, value in enumerate(along(tensor, m)):
                    part[t, i, c] = value
                return inside

            lax.fori_loop(0, steps, block, 0, unroll=True)
            return carry

        lax.fori_loop(first, stop, body, 0)

    def right_fields(win, with_own):
        sources = 3 if with_own else 2

        def work(t, cols):
            lines = [
                jnp.broadcast_to(win[pl.ds(c * tiles + t, 1), :], (2 * ROWS, 128))
                for c in range(3)
            ]
            split = split_lines(lines)
            scalar = jnp.dot(
                jnp.concatenate([split, split], axis=1), scalar_t[t], preferred_element_type=F32
            )[0:ROWS]

            def block(i, sums):
                m = [cols[i, c] for c in range(3)]
                new = []
                for e in range(sources):
                    tensor = [own_t[t, i, c] if e == 2 else pair_t[t, e, i, c] for c in range(3)]
                    new += list(along(tensor, m))
                return tuple(a + b for a, b in zip(sums, new))

            zeros = (jnp.zeros((ROWS, 128), F32),) * (3 * sources)
            sums = lax.fori_loop(0, steps, block, zeros, unroll=True)
            for c in range(3):
                less = [jnp.where(lines_of[c], scalar[:, lanes(e)], 0.0) for e in range(3)]
                own = sums[6 + c] - less[2] if with_own else -less[2]
                own_rows[pl.ds(c * tiles + t, 1), :] = jnp.sum(own, axis=0, keepdims=True)
                for e in range(2):
                    right_rows[pl.ds(2 * tiles * c + 2 * t + e, 1), :] = jnp.sum(
                        sums[3 * e + c] - less[e], axis=0, keepdims=True
                    )

        in_pairs(win, 3, work)
        rows = right_rows[...]
        rows = jnp.concatenate(
            [rows[2 * tiles * c : 2 * tiles * (c + 1)] for c in range(3)], axis=1
        )
        first = rows.astype(jnp.bfloat16)
        rows = rows - first.astype(F32)
        second = rows.astype(jnp.bfloat16)
        third = (rows - second.astype(F32)).astype(jnp.bfloat16)
        split = jnp.concatenate([first, second, third], axis=0)
        total = jnp.dot(hot[...], split, preferred_element_type=F32)
        return [
            jnp.concatenate([half[:, lanes(c)] for c in range(3)], axis=0)
            for half in (total[0:tiles], total[tiles : 2 * tiles])
        ]

    full_lane = lax.broadcasted_iota(jnp.int32, (128, 128), 1)

    def gather_column(t):
        now = colmat[...]
        for c in range(3):
            total = jnp.sum(part[t, :, c].reshape(128, 128), axis=1, keepdims=True)
            now = jnp.where(full_lane == c * tiles + t, total, now)
        colmat[...] = now

    def left_fields(win, with_part):
        def one(t):
            gather_column(lax.rem(t + tiles - 1, tiles))
            m = []
            for e in range(2):
                n = list_ref[e + 1, t]
                first = n + jnp.where(n >= tiles, 2 * tiles, 0)
                m.append(
                    [
                        jnp.broadcast_to(win[pl.ds(first + c * tiles, 1), :], (2 * ROWS, 128))
                        for c in range(3)
                    ]
                )
            scalar = lax.dot_general(
                jnp.concatenate([split_lines(lines) for lines in m], axis=1),
                scalar_t[t, :, 0:256],
                (((1,), (1,)), ((), ())),
                preferred_element_type=F32,
            )[0:ROWS]
            scalar = scalar[:, lanes(0)] + scalar[:, lanes(1)]
            for c in range(3):
                left_rows[pl.ds(c * tiles + t, 1), :] = jnp.sum(
                    jnp.where(lines_of[c], scalar, 0.0), axis=0, keepdims=True
                )
            m = [[line[0:ROWS] for line in lines] for lines in m]

            def block(i, inside):
                sums = [part[t, i, c] for c in range(3)] if with_part else None
                for e in range(2):
                    tensor = [pair_t[t, e, i, c] for c in range(3)]
                    new = along(tensor, m[e])
                    sums = new if sums is None else [a + b for a, b in zip(sums, new)]
                for c in range(3):
                    part[t, i, c] = sums[c]
                return inside

            lax.fori_loop(0, steps, block, 0, unroll=True)

        def body(u, carry):
            for step in range(4):
                one(4 * u + step)
            return carry

        lax.fori_loop(0, tiles // 4, body, 0)
        gather_column(tiles - 1)
        return colmat[...].T[0 : 3 * tiles] - left_rows[...]

    in_pairs(win_p, 4, own_tensors, 0, tiles // 2)

    pl.semaphore_wait(barrier, len(everyone))
    own_p, own_v = 4 * tiles, 3 * tiles
    halo_p = ring_copy(win_p.at[0:own_p], win_p.at[own_p : 2 * own_p], 0, before)
    halo_p.start()
    halos = [
        ring_copy(win.at[0:own_v], win.at[own_v : 2 * own_v], 1 + k, before)
        for k, win in enumerate(wins)
    ]
    returns = [
        ring_copy(ret_out.at[k], ret_in.at[k], 1 + ITERS + k, after) for k in range(ITERS)
    ]
    halos[0].start()
    sum_start(0, 0, packed_sums(gram[0:16, :]))

    in_pairs(win_p, 4, own_tensors, tiles // 2, tiles)
    own_fields(win_0)

    hot_lane = lax.broadcasted_iota(jnp.int32, (1, 128), 1)

    def mark(t, carry):
        for e in range(2):
            value = jnp.where(hot_lane == list_ref[e + 1, t], 1.0, 0.0)
            gram[pl.ds(2 * t + e, 1), :] = value
        return carry

    lax.fori_loop(0, tiles, mark, 0)
    marks = gram[...].T[0 : 2 * tiles, 0 : 2 * tiles].astype(jnp.bfloat16)
    hot[...] = jnp.concatenate([marks] * 3, axis=1)
    gram[...] = jnp.zeros((128, 128), F32)
    slot_ref[...] = inverse_order(atom_ref[...])

    halo_p.wait()
    in_pairs(win_p, 4, pair_tensors)
    sum_start(0, 1, sum_finish(0, 0))

    def own_vector(k):
        return wins[k][0:own_v, :]

    pair_index = {}

    def keep(key, line):
        index = pair_index[key] = len(pair_index)
        gram[index : index + 1, :] = line

    centre = None
    for k in range(ITERS):
        final = k + 1 == ITERS
        if k > 0:
            for j in range(k + 1):
                keep((j, k), inner_rows(own_vector(j), own_vector(k)))
            halos[k].start()
        kept, sent = right_fields(wins[k], final)
        ret_out[k] = sent
        if k > 0 and not final:
            own_fields(wins[k], 0, 4)
        if final:
            now = own_vector(k)
            line = inner_rows(now, shifted * now - (own_rows[...] + 2.0 * kept))
        kept = kept + own_rows[...]
        returns[k].start()
        if k > 0 and not final:
            own_fields(wins[k], 4, tiles)
        halos[k].wait()
        if final:
            line = line - 2.0 * inner_rows(wins[k][own_v : 2 * own_v, :], sent)
            keep((k, k + 1), line)
            sum_start(1, 0, packed_sums(gram[0:16, :]))
        field = left_fields(wins[k], not final) + kept
        if k == 0:
            unpacked(sum_finish(0, 1))
            centre = gram[1:2, :] / gram[0:1, :]
            gram[...] = jnp.zeros((128, 128), F32)
            keep((0, 0), inner_rows(rhs, rhs))
            shifted = jnp.concatenate([inv_alpha - centre] * 3, axis=0)
        if final:
            sum_start(1, 1, sum_finish(1, 0))
        returns[k].wait()
        new = shifted * own_vector(k) - (field + ret_in[k])
        if final:
            top[...] = new
        else:
            wins[k + 1][0:own_v, :] = new

    unpacked(sum_finish(1, 1))
    vectors = [own_vector(k) for k in range(ITERS)] + [top[...]]
    for j in range(ITERS - 1):
        pair_index[(j, ITERS)] = pair_index[(j + 1, ITERS - 1)]

    def entry(a, b):
        index = pair_index[(min(a, b), max(a, b))]
        return gram[index : index + 1, :]

    def form(a, b):
        out = None
        for i, p in enumerate(a):
            for j, q in enumerate(b):
                term = p * q * entry(i, j)
                out = term if out is None else out + term
        return out

    def plus(a, scale, b):
        out = []
        for i in range(max(len(a), len(b))):
            term = scale * b[i] if i < len(b) else None
            if i < len(a):
                out.append(a[i] if term is None else a[i] + term)
            else:
                out.append(term)
        return out

    one = jnp.ones((1, 128), F32)
    x_coef = []
    r_coef = [one]
    d_coef = [one]
    norm_now = form(r_coef, r_coef)
    for iteration in range(ITERS):
        applied = [centre * v for v in d_coef] + [0.0 * one]
        applied = [
            applied[i] + d_coef[i - 1] if i > 0 else applied[i] for i in range(len(applied))
        ]
        step = norm_now / form(d_coef, applied)
        x_coef = plus(x_coef, step, d_coef)
        r_coef = plus(r_coef, -step, applied)
        if iteration + 1 < ITERS:
            norm_next = form(r_coef, r_coef)
            d_coef = plus(r_coef, norm_next / norm_now, d_coef)
            norm_now = norm_next

    for out_ref, coef in ((x_ref, x_coef), (r_ref, r_coef)):
        total = None
        for j, value in enumerate(coef):
            term = value * vectors[j]
            total = term if total is None else total + term
        out_ref[...] = total


def on_device(group, positions, polar, field_ext, tile_atom, tile_list, image_shift):
    atoms = tile_atom.shape[0]
    tiles = tile_list.shape[0]
    inner = 16 if group % 16 == 0 else 2
    outer = group // inner
    steps = 128 // ROWS
    vmem = pl.BlockSpec(memory_space=pltpu.VMEM)
    smem = pl.BlockSpec(memory_space=pltpu.SMEM)
    state = jax.ShapeDtypeStruct((3 * tiles, 128), F32)

    def shape(*dims, dtype=F32):
        return jax.ShapeDtypeStruct(dims, dtype)

    sum_count = 2 * (inner + outer)
    ring_count = 1 + 2 * ITERS
    x, r, slot = pl.pallas_call(
        functools.partial(solve_kernel, group, inner),
        out_shape=(state, state, shape(tiles, 128, dtype=jnp.int32)),
        in_specs=[vmem] * 4 + [smem] * 2,
        out_specs=(vmem,) * 3,
        scratch_shapes=[
            pltpu.VMEM((tiles, 128), F32),
            pltpu.VMEM((tiles, steps, 3, ROWS, 128), F32),
            pltpu.VMEM((tiles, 2, steps, 3, ROWS, 128), F32),
            pltpu.VMEM((tiles, steps, 3, ROWS, 128), F32),
            pltpu.VMEM((steps, 4, ROWS, 128), F32),
            pltpu.VMEM((steps, 4, ROWS, 128), F32),
            pltpu.VMEM((8 * tiles, 128), F32),
        ]
        + [pltpu.VMEM((6 * tiles, 128), F32)] * ITERS
        + [
            pltpu.VMEM((3 * tiles, 128), F32),
            pltpu.VMEM((ITERS, 3 * tiles, 128), F32),
            pltpu.VMEM((ITERS, 3 * tiles, 128), F32),
            pltpu.VMEM((6 * tiles, 128), F32),
            pltpu.VMEM((3 * tiles, 128), F32),
            pltpu.VMEM((3 * tiles, 128), F32),
            pltpu.VMEM((tiles, 256, 384), jnp.bfloat16),
            pltpu.VMEM((2 * tiles, 6 * tiles), jnp.bfloat16),
            pltpu.VMEM((128, 128), F32),
            pltpu.VMEM((128, 128), F32),
            pltpu.VMEM((2, inner, 1, 128), F32),
            pltpu.VMEM((2, outer, 1, 128), F32),
            pltpu.SemaphoreType.DMA((ring_count,)),
            pltpu.SemaphoreType.DMA((ring_count,)),
            pltpu.SemaphoreType.DMA((sum_count,)),
            pltpu.SemaphoreType.DMA((sum_count,)),
        ],
        compiler_params=pltpu.CompilerParams(
            collective_id=0, has_side_effects=True, vmem_limit_bytes=60 * 1024 * 1024
        ),
        name="solve",
    )(
        positions,
        polar.reshape(tiles, 128),
        field_ext,
        tile_atom.reshape(tiles, 128),
        tile_list.T,
        image_shift.transpose(2, 0, 1),
    )

    return pl.pallas_call(
        atom_order_kernel,
        out_shape=(shape(3, atoms), shape(3, atoms)),
        in_specs=[vmem] * 3,
        out_specs=(vmem,) * 2,
        name="atom_order",
    )(x, r, slot)


def solution(mesh):
    both = ("rep", "gx")
    return jax.shard_map(
        functools.partial(on_device, mesh.shape["gx"]),
        mesh=mesh,
        in_specs=(
            P(None, both),
            P(both),
            P(None, both),
            P(both),
            P(both, None),
            P(None, both, None),
        ),
        out_specs=(P(None, both), P(None, both)),
        check_vma=False,
    )
```

```python
import functools
import math

import jax
import jax.numpy as jnp
from jax import lax
from jax.experimental import pallas as pl
from jax.experimental.pallas import tpu as pltpu
from jax.sharding import PartitionSpec as P

ITERS = 4
MESH = pl.DeviceIdType.MESH
THOLE = 0.39
F32 = jnp.float32
ROWS = 8


def lanes(index):
    return slice(index * 128, (index + 1) * 128)


def gathered(slot, rows_at, count, steps):
    blocks = []
    for start in range(0, slot.shape[0], 8):
        index = slot[start : start + 8]
        high = lax.shift_right_logical(index, 7)
        low = jnp.bitwise_and(index, 127)

        def pick(step, found):
            hit = high == step
            return tuple(
                jnp.where(
                    hit,
                    jnp.take_along_axis(jnp.broadcast_to(row, (8, 128)), low, axis=1),
                    old,
                )
                for row, old in zip(rows_at(step), found)
            )

        zero = jnp.zeros((8, 128), F32)
        blocks.append(lax.fori_loop(0, steps, pick, (zero,) * count, unroll=True))
    return blocks


def inverse_order(atom):
    tiles = atom.shape[0]
    high_ids = lax.broadcasted_iota(jnp.int32, (tiles, 128), 0)
    low_ids = lax.broadcasted_iota(jnp.int32, (128, 128), 0)
    lane_ids = lax.broadcasted_iota(jnp.int32, (tiles, 128), 1).astype(F32)
    high = lax.shift_right_logical(atom, 7)
    low = jnp.bitwise_and(atom, 127)
    total = None
    for pair in range(0, tiles, 2):
        left, right = [], []
        for step in (pair, pair + 1):
            hot = high_ids == high[step : step + 1]
            left.append(
                jnp.concatenate(
                    [jnp.where(hot, float(step), 0.0), jnp.where(hot, lane_ids, 0.0)], axis=0
                )
            )
            right.append(jnp.where(low_ids == low[step : step + 1], 1.0, 0.0))
        term = lax.dot_general(
            jnp.concatenate(left, axis=1).astype(jnp.bfloat16),
            jnp.concatenate(right, axis=1).astype(jnp.bfloat16),
            (((1,), (1,)), ((), ())),
            preferred_element_type=F32,
        )
        total = term if total is None else total + term
    return (total[:tiles] * 128.0 + total[tiles:]).astype(jnp.int32)


def atom_order_kernel(x_ref, r_ref, slot_ref, dipoles_ref, residual_ref):
    tiles = slot_ref.shape[0]

    def rows_at(step):
        return [ref[pl.ds(c * tiles + step, 1), :] for ref in (x_ref, r_ref) for c in range(3)]

    for block, found in enumerate(gathered(slot_ref[...], rows_at, 6, tiles)):
        for c in range(3):
            for h in range(8):
                dipoles_ref[c : c + 1, lanes(8 * block + h)] = found[c][h : h + 1, :]
                residual_ref[c : c + 1, lanes(8 * block + h)] = found[3 + c][h : h + 1, :]


def pair_tensor(left, right, diagonal):
    dx = right[0] - left[0]
    dy = right[1] - left[1]
    dz = right[2] - left[2]
    square = dx * dx + dy * dy + dz * dz
    if diagonal is not None:
        square = jnp.where(diagonal, 1.0, square)
    inv = lax.rsqrt(square)
    minus_u = square * (square * inv) * (left[3] * right[3])
    decay = jnp.exp(minus_u)
    inv_cube = inv * (inv * inv)
    rest = 1.0 - decay
    g3 = rest * inv_cube
    if diagonal is not None:
        g3 = jnp.where(diagonal, 0.0, g3)
    damped = (rest + minus_u * decay) * inv_cube
    scale = (damped * lax.rsqrt(damped)) * (inv * math.sqrt(3.0))
    return (dx * scale, dy * scale, dz * scale), g3


def along(e, m):
    share = e[0] * m[0] + e[1] * m[1] + e[2] * m[2]
    return (e[0] * share, e[1] * share, e[2] * share)


def solve_kernel(
    group,
    inner,
    pos_ref,
    polar_ref,
    field_ref,
    atom_ref,
    list_ref,
    shift_ref,
    x_ref,
    r_ref,
    slot_ref,
    inv_alpha_ref,
    own_t,
    pair_t,
    part,
    cols_a,
    cols_b,
    cols_c,
    cols_d,
    win_p,
    win_0,
    win_1,
    win_2,
    win_3,
    top,
    ret_out,
    ret_in,
    right_rows,
    own_rows,
    left_rows,
    scalar_t,
    hot,
    colmat,
    gram,
    sums_1,
    sums_2,
    ring_send,
    ring_recv,
    sum_send,
    sum_recv,
):
    tiles = atom_ref.shape[0]
    me = lax.axis_index("gx")
    outer = group // inner
    row, col = me // inner, me % inner
    after = lax.rem(me + 1, group)
    before = lax.rem(me + group - 1, group)
    peers_1 = [row * inner + lax.rem(col + d, inner) for d in range(1, inner)]
    peers_2 = [lax.rem(row + d, outer) * inner + col for d in range(1, outer)]
    wins = (win_0, win_1, win_2, win_3)
    cols = (cols_a, cols_b, cols_c, cols_d)

    barrier = pltpu.get_barrier_semaphore()
    everyone = [after, before] + peers_1 + peers_2
    for peer in everyone:
        pl.semaphore_signal(barrier, inc=1, device_id={"gx": peer}, device_id_type=MESH)

    def ring_copy(src, dst, index, peer):
        return pltpu.make_async_remote_copy(
            src_ref=src,
            dst_ref=dst,
            send_sem=ring_send.at[index],
            recv_sem=ring_recv.at[index],
            device_id={"gx": peer},
            device_id_type=MESH,
        )

    def sum_copies(which, stage):
        buf = sums_1 if stage == 0 else sums_2
        at = col if stage == 0 else row
        peers = peers_1 if stage == 0 else peers_2
        base = which * (inner + outer) + stage * inner
        return [
            pltpu.make_async_remote_copy(
                src_ref=buf.at[which, at],
                dst_ref=buf.at[which, at],
                send_sem=sum_send.at[base + d],
                recv_sem=sum_recv.at[base + d],
                device_id={"gx": peer},
                device_id_type=MESH,
            )
            for d, peer in enumerate(peers)
        ]

    def sum_start(which, stage, value):
        buf = sums_1 if stage == 0 else sums_2
        buf[which, pl.ds(col if stage == 0 else row, 1)] = value[None]
        for copy in sum_copies(which, stage):
            copy.start()

    def sum_finish(which, stage):
        for copy in sum_copies(which, stage):
            copy.wait()
        buf = sums_1 if stage == 0 else sums_2
        total = buf[which, 0]
        for d in range(1, inner if stage == 0 else outer):
            total = total + buf[which, d]
        return total

    def inner_rows(a, b):
        return jnp.sum(a * b, axis=0, keepdims=True)

    sub_ids = lax.broadcasted_iota(jnp.int32, (16, 128), 0)
    lane_ids = lax.broadcasted_iota(jnp.int32, (16, 128), 1)

    def packed_sums(stack):
        totals = jnp.sum(stack, axis=1, keepdims=True)
        return jnp.sum(jnp.where(sub_ids == lane_ids, totals, 0.0), axis=0, keepdims=True)

    def unpacked(sums):
        gram[...] = jnp.broadcast_to(sums, (128, 128)).T

    def rows_at(ref):
        def rows(step):
            places = pl.ds(pl.multiple_of(step * 128, 128), 128)
            return [ref[c : c + 1, places] for c in range(3)]

        return rows

    def place_rows(step):
        return rows_at(pos_ref)(step) + [polar_ref[pl.ds(step, 1), :]]

    for block, found in enumerate(gathered(atom_ref[...], place_rows, 4, tiles)):
        for c in range(3):
            at = c * tiles + 8 * block
            win_p[at : at + 8, :] = found[c]
        at = 3 * tiles + 8 * block
        win_p[at : at + 8, :] = lax.rsqrt(found[3])
        inv_alpha_ref[8 * block : 8 * block + 8, :] = 1.0 / found[3]

    steps = 128 // ROWS

    def spread(buf, ref, index, count):
        for c in range(count):
            line = ref[pl.ds(c * tiles + index, 1), :]
            buf[:, c] = jnp.broadcast_to(line, (128, 128)).T.reshape(steps, ROWS, 128)

    def right_lines(n, vector):
        first = n + jnp.where(n >= tiles, 3 * tiles, 0)
        lines = [win_p[pl.ds(first + c * tiles, 1), :] for c in range(4)]
        if vector is not None:
            lines = [lines[c] + vector[c] for c in range(3)] + lines[3:]
        lines[3] = lines[3] * (-THOLE)
        return [jnp.broadcast_to(line, (2 * ROWS, 128)) for line in lines]

    sub_16 = lax.broadcasted_iota(jnp.int32, (2 * ROWS, 128), 0)
    lane_16 = lax.broadcasted_iota(jnp.int32, (2 * ROWS, 128), 1)
    sub_8 = lax.broadcasted_iota(jnp.int32, (ROWS, 128), 0)
    lines_of = [jnp.logical_or(sub_8 == c, sub_8 == c + 3) for c in range(3)]
    halves = [jnp.logical_or(sub_16 == c, sub_16 == c + 3) for c in range(3)]

    def tensors(t, cols, right, diagonal, where, place):
        def block(i, carry):
            left = [cols[pl.ds(2 * i, 2), c].reshape(2 * ROWS, 128) for c in range(4)]
            same = sub_16 + i * (2 * ROWS) == lane_16 if diagonal else None
            e, g3 = pair_tensor(left, right, same)
            for c in range(3):
                where(t, i, c, e[c].reshape(2, ROWS, 128))
            high = g3.astype(jnp.bfloat16)
            low = (g3 - high.astype(F32)).astype(jnp.bfloat16)
            at = pl.multiple_of(i * (2 * ROWS), 2 * ROWS)
            scalar_t[t, pl.ds(at, 2 * ROWS), lanes(place)] = high
            scalar_t[t, pl.ds(128 + at, 2 * ROWS), lanes(place)] = low
            return carry

        lax.fori_loop(0, steps // 2, block, 0, unroll=True)

    def own_tensors(t, cols):
        def where(t, i, c, value):
            own_t[t, pl.ds(2 * i, 2), c] = value

        tensors(t, cols, right_lines(t, None), True, where, 2)

    def split_lines(lines):
        wide = jnp.where(halves[0], lines[0], jnp.where(halves[1], lines[1], lines[2]))
        high = wide.astype(jnp.bfloat16).astype(F32)
        return jnp.where(sub_16 < 3, high, wide - high).astype(jnp.bfloat16)

    last = me == group - 1

    def pair_tensors(t, cols):
        for e in range(2):
            n = list_ref[e + 1, t]
            wrap = jnp.where(jnp.logical_and(n >= tiles, last), 4.0 * group, 0.0)
            vector = (
                wrap,
                shift_ref[e + 1, 0, t].astype(F32) * 128.0,
                shift_ref[e + 1, 1, t].astype(F32) * (2.0 * tiles),
            )

            def where(t, i, c, value, e=e):
                pair_t[t, e, pl.ds(2 * i, 2), c] = value

            tensors(t, cols, right_lines(n, vector), False, where, e)

    def in_pairs(ref, count, work, first=0, stop=tiles):
        spread(cols[0], ref, first, count)

        def body(u, carry):
            t = first + 2 * u
            spread(cols[1], ref, t + 1, count)
            work(t, cols[0])
            spread(cols[0], ref, lax.rem(t + 2, tiles), count)
            work(t + 1, cols[1])
            return carry

        lax.fori_loop(0, (stop - first) // 2, body, 0)

    def own_fields(win, first=0, stop=tiles):
        def body(t, carry):
            m = [
                jnp.broadcast_to(win[pl.ds(c * tiles + t, 1), :], (ROWS, 128))
                for c in range(3)
            ]

            def block(i, inside):
                tensor = [own_t[t, i, c] for c in range(3)]
                for c, value in enumerate(along(tensor, m)):
                    part[t, i, c] = value
                return inside

            lax.fori_loop(0, steps, block, 0, unroll=True)
            return carry

        lax.fori_loop(first, stop, body, 0)

    def in_fours(ref, count, work):
        for slot, buf in enumerate(cols[0:2]):
            spread(buf, ref, slot, count)

        def body(u, carry):
            t = 4 * u
            for half in range(2):
                for step in range(2):
                    ahead = lax.rem(t + 2 * half + 2 + step, tiles)
                    spread(cols[2 * (1 - half) + step], ref, ahead, count)
                    work(t + 2 * half + step, cols[2 * half + step])
            return carry

        lax.fori_loop(0, tiles // 4, body, 0)

    def right_fields(win, with_own):
        sources = 3 if with_own else 2

        def work(t, cols):
            lines = [
                jnp.broadcast_to(win[pl.ds(c * tiles + t, 1), :], (2 * ROWS, 128))
                for c in range(3)
            ]
            split = split_lines(lines)
            scalar = jnp.dot(
                jnp.concatenate([split, split], axis=1), scalar_t[t], preferred_element_type=F32
            )[0:ROWS]

            def block(i, sums):
                m = [cols[i, c] for c in range(3)]
                new = []
                for e in range(sources):
                    tensor = [own_t[t, i, c] if e == 2 else pair_t[t, e, i, c] for c in range(3)]
                    new += list(along(tensor, m))
                return tuple(a + b for a, b in zip(sums, new))

            zeros = (jnp.zeros((ROWS, 128), F32),) * (3 * sources)
            sums = lax.fori_loop(0, steps, block, zeros, unroll=True)
            for c in range(3):
                less = [jnp.where(lines_of[c], scalar[:, lanes(e)], 0.0) for e in range(3)]
                own = sums[6 + c] - less[2] if with_own else -less[2]
                own_rows[pl.ds(c * tiles + t, 1), :] = jnp.sum(own, axis=0, keepdims=True)
                for e in range(2):
                    right_rows[pl.ds(2 * tiles * c + 2 * t + e, 1), :] = jnp.sum(
                        sums[3 * e + c] - less[e], axis=0, keepdims=True
                    )

        in_fours(win, 3, work)
        rows = right_rows[...]
        rows = jnp.concatenate(
            [rows[2 * tiles * c : 2 * tiles * (c + 1)] for c in range(3)], axis=1
        )
        first = rows.astype(jnp.bfloat16)
        rows = rows - first.astype(F32)
        second = rows.astype(jnp.bfloat16)
        third = (rows - second.astype(F32)).astype(jnp.bfloat16)
        split = jnp.concatenate([first, second, third], axis=0)
        total = jnp.dot(hot[...], split, preferred_element_type=F32)
        return [
            jnp.concatenate([half[:, lanes(c)] for c in range(3)], axis=0)
            for half in (total[0:tiles], total[tiles : 2 * tiles])
        ]

    full_lane = lax.broadcasted_iota(jnp.int32, (128, 128), 1)

    def gather_column(t):
        now = colmat[...]
        for c in range(3):
            total = jnp.sum(part[t, :, c].reshape(128, 128), axis=1, keepdims=True)
            now = jnp.where(full_lane == c * tiles + t, total, now)
        colmat[...] = now

    def left_fields(win, with_part):
        def one(t):
            gather_column(lax.rem(t + tiles - 1, tiles))
            m = []
            for e in range(2):
                n = list_ref[e + 1, t]
                first = n + jnp.where(n >= tiles, 2 * tiles, 0)
                m.append(
                    [
                        jnp.broadcast_to(win[pl.ds(first + c * tiles, 1), :], (2 * ROWS, 128))
                        for c in range(3)
                    ]
                )
            scalar = lax.dot_general(
                jnp.concatenate([split_lines(lines) for lines in m], axis=1),
                scalar_t[t, :, 0:256],
                (((1,), (1,)), ((), ())),
                preferred_element_type=F32,
            )[0:ROWS]
            scalar = scalar[:, lanes(0)] + scalar[:, lanes(1)]
            for c in range(3):
                left_rows[pl.ds(c * tiles + t, 1), :] = jnp.sum(
                    jnp.where(lines_of[c], scalar, 0.0), axis=0, keepdims=True
                )
            m = [[line[0:ROWS] for line in lines] for lines in m]

            def block(i, inside):
                sums = [part[t, i, c] for c in range(3)] if with_part else None
                for e in range(2):
                    tensor = [pair_t[t, e, i, c] for c in range(3)]
                    new = along(tensor, m[e])
                    sums = new if sums is None else [a + b for a, b in zip(sums, new)]
                for c in range(3):
                    part[t, i, c] = sums[c]
                return inside

            lax.fori_loop(0, steps, block, 0, unroll=True)

        def body(u, carry):
            for step in range(8):
                one(8 * u + step)
            return carry

        lax.fori_loop(0, tiles // 8, body, 0)
        gather_column(tiles - 1)
        return colmat[...].T[0 : 3 * tiles] - left_rows[...]

    in_pairs(win_p, 4, own_tensors, 0, tiles // 2)

    pl.semaphore_wait(barrier, len(everyone))
    own_p, own_v = 4 * tiles, 3 * tiles
    halo_p = ring_copy(win_p.at[0:own_p], win_p.at[own_p : 2 * own_p], 0, before)
    halo_p.start()

    for block, found in enumerate(gathered(atom_ref[...], rows_at(field_ref), 3, tiles)):
        for c in range(3):
            at = c * tiles + 8 * block
            win_0[at : at + 8, :] = found[c]

    rhs = win_0[0 : 3 * tiles, :]
    inv_alpha = inv_alpha_ref[...]
    inv_alpha_3 = jnp.concatenate([inv_alpha] * 3, axis=0)
    colmat[...] = jnp.zeros((128, 128), F32)
    gram[...] = jnp.zeros((128, 128), F32)
    gram[0:1, :] = inner_rows(rhs, rhs)
    gram[1:2, :] = inner_rows(rhs, rhs * inv_alpha_3)

    halos = [
        ring_copy(win.at[0:own_v], win.at[own_v : 2 * own_v], 1 + k, before)
        for k, win in enumerate(wins)
    ]
    returns = [
        ring_copy(ret_out.at[k], ret_in.at[k], 1 + ITERS + k, after) for k in range(ITERS)
    ]
    halos[0].start()
    sum_start(0, 0, packed_sums(gram[0:16, :]))

    in_pairs(win_p, 4, own_tensors, tiles // 2, tiles)
    own_fields(win_0)

    hot_lane = lax.broadcasted_iota(jnp.int32, (1, 128), 1)

    def mark(t, carry):
        for e in range(2):
            value = jnp.where(hot_lane == list_ref[e + 1, t], 1.0, 0.0)
            gram[pl.ds(2 * t + e, 1), :] = value
        return carry

    lax.fori_loop(0, tiles, mark, 0)
    marks = gram[...].T[0 : 2 * tiles, 0 : 2 * tiles].astype(jnp.bfloat16)
    hot[...] = jnp.concatenate([marks] * 3, axis=1)
    gram[...] = jnp.zeros((128, 128), F32)
    slot_ref[...] = inverse_order(atom_ref[...])

    halo_p.wait()
    in_pairs(win_p, 4, pair_tensors)
    sum_start(0, 1, sum_finish(0, 0))

    def own_vector(k):
        return wins[k][0:own_v, :]

    pair_index = {}

    def keep(key, line):
        index = pair_index[key] = len(pair_index)
        gram[index : index + 1, :] = line

    centre = None
    for k in range(ITERS):
        final = k + 1 == ITERS
        if k > 0:
            for j in range(k + 1):
                keep((j, k), inner_rows(own_vector(j), own_vector(k)))
            halos[k].start()
        kept, sent = right_fields(wins[k], final)
        ret_out[k] = sent
        if k > 0 and not final:
            own_fields(wins[k], 0, 4)
        if final:
            now = own_vector(k)
            line = inner_rows(now, shifted * now - (own_rows[...] + 2.0 * kept))
        kept = kept + own_rows[...]
        returns[k].start()
        if k > 0 and not final:
            own_fields(wins[k], 4, tiles)
        halos[k].wait()
        if final:
            line = line - 2.0 * inner_rows(wins[k][own_v : 2 * own_v, :], sent)
            keep((k, k + 1), line)
            sum_start(1, 0, packed_sums(gram[0:16, :]))
        field = left_fields(wins[k], not final) + kept
        if k == 0:
            unpacked(sum_finish(0, 1))
            centre = gram[1:2, :] / gram[0:1, :]
            gram[...] = jnp.zeros((128, 128), F32)
            keep((0, 0), inner_rows(rhs, rhs))
            shifted = jnp.concatenate([inv_alpha - centre] * 3, axis=0)
        if final:
            sum_start(1, 1, sum_finish(1, 0))
        returns[k].wait()
        new = shifted * own_vector(k) - (field + ret_in[k])
        if final:
            top[...] = new
        else:
            wins[k + 1][0:own_v, :] = new

    unpacked(sum_finish(1, 1))
    vectors = [own_vector(k) for k in range(ITERS)] + [top[...]]
    for j in range(ITERS - 1):
        pair_index[(j, ITERS)] = pair_index[(j + 1, ITERS - 1)]

    def entry(a, b):
        index = pair_index[(min(a, b), max(a, b))]
        return gram[index : index + 1, :]

    def form(a, b):
        out = None
        for i, p in enumerate(a):
            for j, q in enumerate(b):
                term = p * q * entry(i, j)
                out = term if out is None else out + term
        return out

    def plus(a, scale, b):
        out = []
        for i in range(max(len(a), len(b))):
            term = scale * b[i] if i < len(b) else None
            if i < len(a):
                out.append(a[i] if term is None else a[i] + term)
            else:
                out.append(term)
        return out

    one = jnp.ones((1, 128), F32)
    x_coef = []
    r_coef = [one]
    d_coef = [one]
    norm_now = form(r_coef, r_coef)
    for iteration in range(ITERS):
        applied = [centre * v for v in d_coef] + [0.0 * one]
        applied = [
            applied[i] + d_coef[i - 1] if i > 0 else applied[i] for i in range(len(applied))
        ]
        step = norm_now / form(d_coef, applied)
        x_coef = plus(x_coef, step, d_coef)
        r_coef = plus(r_coef, -step, applied)
        if iteration + 1 < ITERS:
            norm_next = form(r_coef, r_coef)
            d_coef = plus(r_coef, norm_next / norm_now, d_coef)
            norm_now = norm_next

    for out_ref, coef in ((x_ref, x_coef), (r_ref, r_coef)):
        total = None
        for j, value in enumerate(coef):
            term = value * vectors[j]
            total = term if total is None else total + term
        out_ref[...] = total


def on_device(group, positions, polar, field_ext, tile_atom, tile_list, image_shift):
    atoms = tile_atom.shape[0]
    tiles = tile_list.shape[0]
    inner = 16 if group % 16 == 0 else 2
    outer = group // inner
    steps = 128 // ROWS
    vmem = pl.BlockSpec(memory_space=pltpu.VMEM)
    smem = pl.BlockSpec(memory_space=pltpu.SMEM)

    def shape(*dims, dtype=F32):
        return jax.ShapeDtypeStruct(dims, dtype)

    sum_count = 2 * (inner + outer)
    ring_count = 1 + 2 * ITERS
    x, r, slot = pl.pallas_call(
        functools.partial(solve_kernel, group, inner),
        out_shape=(
            pltpu.VMEM((3 * tiles, 128), F32),
            pltpu.VMEM((3 * tiles, 128), F32),
            pltpu.VMEM((tiles, 128), jnp.int32),
        ),
        in_specs=[vmem] * 4 + [smem] * 2,
        out_specs=(vmem,) * 3,
        scratch_shapes=[
            pltpu.VMEM((tiles, 128), F32),
            pltpu.VMEM((tiles, steps, 3, ROWS, 128), F32),
            pltpu.VMEM((tiles, 2, steps, 3, ROWS, 128), F32),
            pltpu.VMEM((tiles, steps, 3, ROWS, 128), F32),
            pltpu.VMEM((steps, 4, ROWS, 128), F32),
            pltpu.VMEM((steps, 4, ROWS, 128), F32),
            pltpu.VMEM((steps, 3, ROWS, 128), F32),
            pltpu.VMEM((steps, 3, ROWS, 128), F32),
            pltpu.VMEM((8 * tiles, 128), F32),
        ]
        + [pltpu.VMEM((6 * tiles, 128), F32)] * ITERS
        + [
            pltpu.VMEM((3 * tiles, 128), F32),
            pltpu.VMEM((ITERS, 3 * tiles, 128), F32),
            pltpu.VMEM((ITERS, 3 * tiles, 128), F32),
            pltpu.VMEM((6 * tiles, 128), F32),
            pltpu.VMEM((3 * tiles, 128), F32),
            pltpu.VMEM((3 * tiles, 128), F32),
            pltpu.VMEM((tiles, 256, 384), jnp.bfloat16),
            pltpu.VMEM((2 * tiles, 6 * tiles), jnp.bfloat16),
            pltpu.VMEM((128, 128), F32),
            pltpu.VMEM((128, 128), F32),
            pltpu.VMEM((2, inner, 1, 128), F32),
            pltpu.VMEM((2, outer, 1, 128), F32),
            pltpu.SemaphoreType.DMA((ring_count,)),
            pltpu.SemaphoreType.DMA((ring_count,)),
            pltpu.SemaphoreType.DMA((sum_count,)),
            pltpu.SemaphoreType.DMA((sum_count,)),
        ],
        compiler_params=pltpu.CompilerParams(
            collective_id=0, has_side_effects=True, vmem_limit_bytes=60 * 1024 * 1024
        ),
        name="solve",
    )(
        positions,
        polar.reshape(tiles, 128),
        field_ext,
        tile_atom.reshape(tiles, 128),
        tile_list.T,
        image_shift.transpose(2, 0, 1),
    )

    return pl.pallas_call(
        atom_order_kernel,
        out_shape=(shape(3, atoms), shape(3, atoms)),
        in_specs=[vmem] * 3,
        out_specs=(vmem,) * 2,
        name="atom_order",
    )(*(pltpu.with_memory_space_constraint(value, pltpu.VMEM) for value in (x, r, slot)))


def solution(mesh):
    both = ("rep", "gx")
    return jax.shard_map(
        functools.partial(on_device, mesh.shape["gx"]),
        mesh=mesh,
        in_specs=(
            P(None, both),
            P(both),
            P(None, both),
            P(both),
            P(both, None),
            P(None, both, None),
        ),
        out_specs=(P(None, both), P(None, both)),
        check_vma=False,
    )
```

```python
import functools
import math

import jax
import jax.numpy as jnp
from jax import lax
from jax.experimental import pallas as pl
from jax.experimental.pallas import tpu as pltpu
from jax.sharding import PartitionSpec as P

ITERS = 4
MESH = pl.DeviceIdType.MESH
THOLE = 0.39
F32 = jnp.float32
ROWS = 8


def lanes(index):
    return slice(index * 128, (index + 1) * 128)


def gathered(slot, rows_at, count, steps):
    blocks = []
    for start in range(0, slot.shape[0], 8):
        index = slot[start : start + 8]
        high = lax.shift_right_logical(index, 7)
        low = jnp.bitwise_and(index, 127)

        def pick(step, found):
            hit = high == step
            return tuple(
                jnp.where(
                    hit,
                    jnp.take_along_axis(jnp.broadcast_to(row, (8, 128)), low, axis=1),
                    old,
                )
                for row, old in zip(rows_at(step), found)
            )

        zero = jnp.zeros((8, 128), F32)
        blocks.append(lax.fori_loop(0, steps, pick, (zero,) * count, unroll=True))
    return blocks


def inverse_order(atom):
    tiles = atom.shape[0]
    high_ids = lax.broadcasted_iota(jnp.int32, (tiles, 128), 0)
    low_ids = lax.broadcasted_iota(jnp.int32, (128, 128), 0)
    lane_ids = lax.broadcasted_iota(jnp.int32, (tiles, 128), 1).astype(F32)
    high = lax.shift_right_logical(atom, 7)
    low = jnp.bitwise_and(atom, 127)
    total = None
    for pair in range(0, tiles, 2):
        left, right = [], []
        for step in (pair, pair + 1):
            hot = high_ids == high[step : step + 1]
            left.append(
                jnp.concatenate(
                    [jnp.where(hot, float(step), 0.0), jnp.where(hot, lane_ids, 0.0)], axis=0
                )
            )
            right.append(jnp.where(low_ids == low[step : step + 1], 1.0, 0.0))
        term = lax.dot_general(
            jnp.concatenate(left, axis=1).astype(jnp.bfloat16),
            jnp.concatenate(right, axis=1).astype(jnp.bfloat16),
            (((1,), (1,)), ((), ())),
            preferred_element_type=F32,
        )
        total = term if total is None else total + term
    return (total[:tiles] * 128.0 + total[tiles:]).astype(jnp.int32)


def atom_order_kernel(x_ref, r_ref, slot_ref, dipoles_ref, residual_ref):
    tiles = slot_ref.shape[0]

    def rows_at(step):
        return [ref[pl.ds(c * tiles + step, 1), :] for ref in (x_ref, r_ref) for c in range(3)]

    for block, found in enumerate(gathered(slot_ref[...], rows_at, 6, tiles)):
        for c in range(3):
            for h in range(8):
                dipoles_ref[c : c + 1, lanes(8 * block + h)] = found[c][h : h + 1, :]
                residual_ref[c : c + 1, lanes(8 * block + h)] = found[3 + c][h : h + 1, :]


def pair_tensor(left, right, diagonal):
    dx = right[0] - left[0]
    dy = right[1] - left[1]
    dz = right[2] - left[2]
    square = dx * dx + dy * dy + dz * dz
    if diagonal is not None:
        square = jnp.where(diagonal, 1.0, square)
    inv = lax.rsqrt(square)
    minus_u = square * (square * inv) * (left[3] * right[3])
    decay = jnp.exp(minus_u)
    inv_cube = inv * (inv * inv)
    rest = 1.0 - decay
    g3 = rest * inv_cube
    if diagonal is not None:
        g3 = jnp.where(diagonal, 0.0, g3)
    damped = (rest + minus_u * decay) * inv_cube
    scale = (damped * lax.rsqrt(damped)) * (inv * math.sqrt(3.0))
    return (dx * scale, dy * scale, dz * scale), g3


def along(e, m):
    share = e[0] * m[0] + e[1] * m[1] + e[2] * m[2]
    return (e[0] * share, e[1] * share, e[2] * share)


def solve_kernel(
    group,
    inner,
    pos_ref,
    polar_ref,
    field_ref,
    atom_ref,
    list_ref,
    shift_ref,
    lines_ref,
    x_ref,
    r_ref,
    slot_ref,
    inv_alpha_ref,
    own_t,
    pair_t,
    part,
    cols_a,
    cols_b,
    cols_c,
    cols_d,
    win_p,
    win_0,
    win_1,
    win_2,
    win_3,
    top,
    ret_out,
    ret_in,
    right_rows,
    own_rows,
    left_rows,
    scalar_t,
    hot,
    colmat,
    gram,
    sums_1,
    sums_2,
    ring_send,
    ring_recv,
    sum_send,
    sum_recv,
):
    tiles = atom_ref.shape[0]
    me = lax.axis_index("gx")
    outer = group // inner
    row, col = me // inner, me % inner
    after = lax.rem(me + 1, group)
    before = lax.rem(me + group - 1, group)
    peers_1 = [row * inner + lax.rem(col + d, inner) for d in range(1, inner)]
    peers_2 = [lax.rem(row + d, outer) * inner + col for d in range(1, outer)]
    wins = (win_0, win_1, win_2, win_3)
    cols = (cols_a, cols_b, cols_c, cols_d)

    barrier = pltpu.get_barrier_semaphore()
    everyone = [after, before] + peers_1 + peers_2
    for peer in everyone:
        pl.semaphore_signal(barrier, inc=1, device_id={"gx": peer}, device_id_type=MESH)

    def ring_copy(src, dst, index, peer):
        return pltpu.make_async_remote_copy(
            src_ref=src,
            dst_ref=dst,
            send_sem=ring_send.at[index],
            recv_sem=ring_recv.at[index],
            device_id={"gx": peer},
            device_id_type=MESH,
        )

    def sum_copies(which, stage):
        buf = sums_1 if stage == 0 else sums_2
        at = col if stage == 0 else row
        peers = peers_1 if stage == 0 else peers_2
        base = which * (inner + outer) + stage * inner
        return [
            pltpu.make_async_remote_copy(
                src_ref=buf.at[which, at],
                dst_ref=buf.at[which, at],
                send_sem=sum_send.at[base + d],
                recv_sem=sum_recv.at[base + d],
                device_id={"gx": peer},
                device_id_type=MESH,
            )
            for d, peer in enumerate(peers)
        ]

    def sum_start(which, stage, value):
        buf = sums_1 if stage == 0 else sums_2
        buf[which, pl.ds(col if stage == 0 else row, 1)] = value[None]
        for copy in sum_copies(which, stage):
            copy.start()

    def sum_finish(which, stage):
        for copy in sum_copies(which, stage):
            copy.wait()
        buf = sums_1 if stage == 0 else sums_2
        total = buf[which, 0]
        for d in range(1, inner if stage == 0 else outer):
            total = total + buf[which, d]
        return total

    def inner_rows(a, b):
        return jnp.sum(a * b, axis=0, keepdims=True)

    sub_ids = lax.broadcasted_iota(jnp.int32, (16, 128), 0)
    lane_ids = lax.broadcasted_iota(jnp.int32, (16, 128), 1)

    def packed_sums(stack):
        totals = jnp.sum(stack, axis=1, keepdims=True)
        return jnp.sum(jnp.where(sub_ids == lane_ids, totals, 0.0), axis=0, keepdims=True)

    def unpacked(sums):
        gram[...] = jnp.broadcast_to(sums, (128, 128)).T

    def rows_at(ref):
        def rows(step):
            places = pl.ds(pl.multiple_of(step * 128, 128), 128)
            return [ref[c : c + 1, places] for c in range(3)]

        return rows

    def place_rows(step):
        return rows_at(pos_ref)(step) + [polar_ref[pl.ds(step, 1), :]]

    for block, found in enumerate(gathered(atom_ref[...], place_rows, 4, tiles)):
        for c in range(3):
            at = c * tiles + 8 * block
            win_p[at : at + 8, :] = found[c]
        at = 3 * tiles + 8 * block
        win_p[at : at + 8, :] = lax.rsqrt(found[3])
        inv_alpha_ref[8 * block : 8 * block + 8, :] = 1.0 / found[3]

    steps = 128 // ROWS

    def spread(buf, ref, index, count):
        for c in range(count):
            line = ref[pl.ds(c * tiles + index, 1), :]
            buf[:, c] = jnp.broadcast_to(line, (128, 128)).T.reshape(steps, ROWS, 128)

    def right_lines(n, vector):
        first = n + jnp.where(n >= tiles, 3 * tiles, 0)
        lines = [win_p[pl.ds(first + c * tiles, 1), :] for c in range(4)]
        if vector is not None:
            lines = [lines[c] + vector[c] for c in range(3)] + lines[3:]
        lines[3] = lines[3] * (-THOLE)
        return [jnp.broadcast_to(line, (2 * ROWS, 128)) for line in lines]

    sub_16 = lax.broadcasted_iota(jnp.int32, (2 * ROWS, 128), 0)
    lane_16 = lax.broadcasted_iota(jnp.int32, (2 * ROWS, 128), 1)
    sub_8 = lax.broadcasted_iota(jnp.int32, (ROWS, 128), 0)
    lines_of = [jnp.logical_or(sub_8 == c, sub_8 == c + 3) for c in range(3)]
    halves = [jnp.logical_or(sub_16 == c, sub_16 == c + 3) for c in range(3)]

    def tensors(t, cols, right, diagonal, where, place):
        def block(i, carry):
            left = [cols[pl.ds(2 * i, 2), c].reshape(2 * ROWS, 128) for c in range(4)]
            same = sub_16 + i * (2 * ROWS) == lane_16 if diagonal else None
            e, g3 = pair_tensor(left, right, same)
            for c in range(3):
                where(t, i, c, e[c].reshape(2, ROWS, 128))
            high = g3.astype(jnp.bfloat16)
            low = (g3 - high.astype(F32)).astype(jnp.bfloat16)
            at = pl.multiple_of(i * (2 * ROWS), 2 * ROWS)
            scalar_t[t, pl.ds(at, 2 * ROWS), lanes(place)] = high
            scalar_t[t, pl.ds(128 + at, 2 * ROWS), lanes(place)] = low
            return carry

        lax.fori_loop(0, steps // 2, block, 0, unroll=True)

    def own_tensors(t, cols):
        def where(t, i, c, value):
            own_t[t, pl.ds(2 * i, 2), c] = value

        tensors(t, cols, right_lines(t, None), True, where, 2)

    def split_lines(lines):
        wide = jnp.where(halves[0], lines[0], jnp.where(halves[1], lines[1], lines[2]))
        high = wide.astype(jnp.bfloat16).astype(F32)
        return jnp.where(sub_16 < 3, high, wide - high).astype(jnp.bfloat16)

    last = me == group - 1

    def pair_tensors(t, cols):
        for e in range(2):
            n = list_ref[e + 1, t]
            wrap = jnp.where(jnp.logical_and(n >= tiles, last), 4.0 * group, 0.0)
            vector = (
                wrap,
                shift_ref[e + 1, 0, t].astype(F32) * 128.0,
                shift_ref[e + 1, 1, t].astype(F32) * (2.0 * tiles),
            )

            def where(t, i, c, value, e=e):
                pair_t[t, e, pl.ds(2 * i, 2), c] = value

            tensors(t, cols, right_lines(n, vector), False, where, e)

    def in_pairs(ref, count, work, first=0, stop=tiles):
        spread(cols[0], ref, first, count)

        def body(u, carry):
            t = first + 2 * u
            spread(cols[1], ref, t + 1, count)
            work(t, cols[0])
            spread(cols[0], ref, lax.rem(t + 2, tiles), count)
            work(t + 1, cols[1])
            return carry

        lax.fori_loop(0, (stop - first) // 2, body, 0)

    def own_fields(win, first=0, stop=tiles):
        def body(t, carry):
            m = [
                jnp.broadcast_to(win[pl.ds(c * tiles + t, 1), :], (ROWS, 128))
                for c in range(3)
            ]

            def block(i, inside):
                tensor = [own_t[t, i, c] for c in range(3)]
                for c, value in enumerate(along(tensor, m)):
                    part[t, i, c] = value
                return inside

            lax.fori_loop(0, steps, block, 0, unroll=True)
            return carry

        lax.fori_loop(first, stop, body, 0)

    def in_fours(ref, count, work):
        for slot, buf in enumerate(cols[0:2]):
            spread(buf, ref, slot, count)

        def body(u, carry):
            t = 4 * u
            for half in range(2):
                for step in range(2):
                    ahead = lax.rem(t + 2 * half + 2 + step, tiles)
                    spread(cols[2 * (1 - half) + step], ref, ahead, count)
                    work(t + 2 * half + step, cols[2 * half + step])
            return carry

        lax.fori_loop(0, tiles // 4, body, 0)

    def right_fields(win, with_own):
        sources = 3 if with_own else 2

        def work(t, cols):
            lines = [
                jnp.broadcast_to(win[pl.ds(c * tiles + t, 1), :], (2 * ROWS, 128))
                for c in range(3)
            ]
            split = split_lines(lines)
            scalar = jnp.dot(
                jnp.concatenate([split, split], axis=1), scalar_t[t], preferred_element_type=F32
            )[0:ROWS]

            def block(i, sums):
                m = [cols[i, c] for c in range(3)]
                new = []
                for e in range(sources):
                    tensor = [own_t[t, i, c] if e == 2 else pair_t[t, e, i, c] for c in range(3)]
                    new += list(along(tensor, m))
                return tuple(a + b for a, b in zip(sums, new))

            zeros = (jnp.zeros((ROWS, 128), F32),) * (3 * sources)
            sums = lax.fori_loop(0, steps, block, zeros, unroll=True)
            for c in range(3):
                less = [jnp.where(lines_of[c], scalar[:, lanes(e)], 0.0) for e in range(3)]
                own = sums[6 + c] - less[2] if with_own else -less[2]
                own_rows[pl.ds(c * tiles + t, 1), :] = jnp.sum(own, axis=0, keepdims=True)
                for e in range(2):
                    right_rows[pl.ds(tiles * (2 * c + e) + t, 1), :] = jnp.sum(
                        sums[3 * e + c] - less[e], axis=0, keepdims=True
                    )

        in_fours(win, 3, work)
        rows = right_rows[...]
        rows = jnp.concatenate(
            [rows[2 * tiles * c : 2 * tiles * (c + 1)] for c in range(3)], axis=1
        )
        first = rows.astype(jnp.bfloat16)
        rows = rows - first.astype(F32)
        second = rows.astype(jnp.bfloat16)
        third = (rows - second.astype(F32)).astype(jnp.bfloat16)
        split = jnp.concatenate([first, second, third], axis=0)
        total = jnp.dot(hot[...], split, preferred_element_type=F32)
        return [
            jnp.concatenate([half[:, lanes(c)] for c in range(3)], axis=0)
            for half in (total[0:tiles], total[tiles : 2 * tiles])
        ]

    full_lane = lax.broadcasted_iota(jnp.int32, (128, 128), 1)

    def gather_column(t):
        now = colmat[...]
        for c in range(3):
            total = jnp.sum(part[t, :, c].reshape(128, 128), axis=1, keepdims=True)
            now = jnp.where(full_lane == c * tiles + t, total, now)
        colmat[...] = now

    def left_fields(win, with_part):
        def one(t):
            gather_column(lax.rem(t + tiles - 1, tiles))
            m = []
            for e in range(2):
                n = list_ref[e + 1, t]
                first = n + jnp.where(n >= tiles, 2 * tiles, 0)
                m.append(
                    [
                        jnp.broadcast_to(win[pl.ds(first + c * tiles, 1), :], (2 * ROWS, 128))
                        for c in range(3)
                    ]
                )
            scalar = lax.dot_general(
                jnp.concatenate([split_lines(lines) for lines in m], axis=1),
                scalar_t[t, :, 0:256],
                (((1,), (1,)), ((), ())),
                preferred_element_type=F32,
            )[0:ROWS]
            scalar = scalar[:, lanes(0)] + scalar[:, lanes(1)]
            for c in range(3):
                left_rows[pl.ds(c * tiles + t, 1), :] = jnp.sum(
                    jnp.where(lines_of[c], scalar, 0.0), axis=0, keepdims=True
                )
            m = [[line[0:ROWS] for line in lines] for lines in m]

            def block(i, inside):
                sums = [part[t, i, c] for c in range(3)] if with_part else None
                for e in range(2):
                    tensor = [pair_t[t, e, i, c] for c in range(3)]
                    new = along(tensor, m[e])
                    sums = new if sums is None else [a + b for a, b in zip(sums, new)]
                for c in range(3):
                    part[t, i, c] = sums[c]
                return inside

            lax.fori_loop(0, steps, block, 0, unroll=True)

        def body(u, carry):
            for step in range(8):
                one(8 * u + step)
            return carry

        lax.fori_loop(0, tiles // 8, body, 0)
        gather_column(tiles - 1)
        return colmat[...].T[0 : 3 * tiles] - left_rows[...]

    in_pairs(win_p, 4, own_tensors, 0, tiles // 4)

    pl.semaphore_wait(barrier, len(everyone))
    own_p, own_v = 4 * tiles, 3 * tiles
    halo_p = ring_copy(win_p.at[0:own_p], win_p.at[own_p : 2 * own_p], 0, before)
    halo_p.start()

    for block, found in enumerate(gathered(atom_ref[...], rows_at(field_ref), 3, tiles)):
        for c in range(3):
            at = c * tiles + 8 * block
            win_0[at : at + 8, :] = found[c]

    rhs = win_0[0 : 3 * tiles, :]
    inv_alpha = inv_alpha_ref[...]
    inv_alpha_3 = jnp.concatenate([inv_alpha] * 3, axis=0)
    colmat[...] = jnp.zeros((128, 128), F32)
    gram[...] = jnp.zeros((128, 128), F32)
    gram[0:1, :] = inner_rows(rhs, rhs)
    gram[1:2, :] = inner_rows(rhs, rhs * inv_alpha_3)

    halos = [
        ring_copy(win.at[0:own_v], win.at[own_v : 2 * own_v], 1 + k, before)
        for k, win in enumerate(wins)
    ]
    returns = [
        ring_copy(ret_out.at[k], ret_in.at[k], 1 + ITERS + k, after) for k in range(ITERS)
    ]
    halos[0].start()
    sum_start(0, 0, packed_sums(gram[0:16, :]))

    in_pairs(win_p, 4, own_tensors, tiles // 4, tiles)
    own_fields(win_0)

    tile_ids = lax.broadcasted_iota(jnp.int32, (2 * tiles, tiles), 0)
    marks = [jnp.where(lines_ref[e : e + 1, :] == tile_ids, 1.0, 0.0) for e in (1, 2)]
    hot[...] = jnp.concatenate(marks * 3, axis=1).astype(jnp.bfloat16)

    halo_p.wait()
    in_pairs(win_p, 4, pair_tensors)
    sum_start(0, 1, sum_finish(0, 0))

    def own_vector(k):
        return wins[k][0:own_v, :]

    pair_index = {}

    def keep(key, line):
        index = pair_index[key] = len(pair_index)
        gram[index : index + 1, :] = line

    centre = None
    for k in range(ITERS):
        final = k + 1 == ITERS
        if k > 0:
            keep((k, k), inner_rows(own_vector(k), own_vector(k)))
            halos[k].start()
            for j in range(k):
                keep((j, k), inner_rows(own_vector(j), own_vector(k)))
        kept, sent = right_fields(wins[k], final)
        ret_out[k] = sent
        if k > 0 and not final:
            own_fields(wins[k], 0, 4)
        if final:
            now = own_vector(k)
            line = inner_rows(now, shifted * now - (own_rows[...] + 2.0 * kept))
        kept = kept + own_rows[...]
        returns[k].start()
        if k > 0 and not final:
            own_fields(wins[k], 4, tiles)
        halos[k].wait()
        if final:
            line = line - 2.0 * inner_rows(wins[k][own_v : 2 * own_v, :], sent)
            keep((k, k + 1), line)
            sum_start(1, 0, packed_sums(gram[0:16, :]))
        field = left_fields(wins[k], not final) + kept
        if k == 0:
            unpacked(sum_finish(0, 1))
            centre = gram[1:2, :] / gram[0:1, :]
            gram[...] = jnp.zeros((128, 128), F32)
            keep((0, 0), inner_rows(rhs, rhs))
            shifted = jnp.concatenate([inv_alpha - centre] * 3, axis=0)
        if final:
            slot_ref[...] = inverse_order(atom_ref[...])
            sum_start(1, 1, sum_finish(1, 0))
        returns[k].wait()
        new = shifted * own_vector(k) - (field + ret_in[k])
        if final:
            top[...] = new
        else:
            wins[k + 1][0:own_v, :] = new

    unpacked(sum_finish(1, 1))
    vectors = [own_vector(k) for k in range(ITERS)] + [top[...]]
    for j in range(ITERS - 1):
        pair_index[(j, ITERS)] = pair_index[(j + 1, ITERS - 1)]

    def entry(a, b):
        index = pair_index[(min(a, b), max(a, b))]
        return gram[index : index + 1, :]

    def form(a, b):
        terms = [p * (q * entry(i, j)) for i, p in enumerate(a) for j, q in enumerate(b)]
        while len(terms) > 1:
            terms = [sum(terms[i + 1 : i + 2], terms[i]) for i in range(0, len(terms), 2)]
        return terms[0]

    def plus(a, scale, b):
        out = []
        for i in range(max(len(a), len(b))):
            term = scale * b[i] if i < len(b) else None
            if i < len(a):
                out.append(a[i] if term is None else a[i] + term)
            else:
                out.append(term)
        return out

    one = jnp.ones((1, 128), F32)
    x_coef = []
    r_coef = [one]
    d_coef = [one]
    norm_now = form(r_coef, r_coef)
    for iteration in range(ITERS):
        applied = [centre * v for v in d_coef] + [0.0 * one]
        applied = [
            applied[i] + d_coef[i - 1] if i > 0 else applied[i] for i in range(len(applied))
        ]
        step = norm_now / form(d_coef, applied)
        x_coef = plus(x_coef, step, d_coef)
        r_coef = plus(r_coef, -step, applied)
        if iteration + 1 < ITERS:
            norm_next = form(r_coef, r_coef)
            d_coef = plus(r_coef, norm_next / norm_now, d_coef)
            norm_now = norm_next

    for out_ref, coef in ((x_ref, x_coef), (r_ref, r_coef)):
        total = None
        for j, value in enumerate(coef):
            term = value * vectors[j]
            total = term if total is None else total + term
        out_ref[...] = total


def on_device(group, positions, polar, field_ext, tile_atom, tile_list, image_shift):
    atoms = tile_atom.shape[0]
    tiles = tile_list.shape[0]
    inner = 16 if group % 16 == 0 else 2
    outer = group // inner
    steps = 128 // ROWS
    vmem = pl.BlockSpec(memory_space=pltpu.VMEM)
    smem = pl.BlockSpec(memory_space=pltpu.SMEM)

    def shape(*dims, dtype=F32):
        return jax.ShapeDtypeStruct(dims, dtype)

    sum_count = 2 * (inner + outer)
    ring_count = 1 + 2 * ITERS
    x, r, slot = pl.pallas_call(
        functools.partial(solve_kernel, group, inner),
        out_shape=(
            pltpu.VMEM((3 * tiles, 128), F32),
            pltpu.VMEM((3 * tiles, 128), F32),
            pltpu.VMEM((tiles, 128), jnp.int32),
        ),
        in_specs=[vmem] * 4 + [smem] * 2 + [vmem],
        out_specs=(vmem,) * 3,
        scratch_shapes=[
            pltpu.VMEM((tiles, 128), F32),
            pltpu.VMEM((tiles, steps, 3, ROWS, 128), F32),
            pltpu.VMEM((tiles, 2, steps, 3, ROWS, 128), F32),
            pltpu.VMEM((tiles, steps, 3, ROWS, 128), F32),
            pltpu.VMEM((steps, 4, ROWS, 128), F32),
            pltpu.VMEM((steps, 4, ROWS, 128), F32),
            pltpu.VMEM((steps, 3, ROWS, 128), F32),
            pltpu.VMEM((steps, 3, ROWS, 128), F32),
            pltpu.VMEM((8 * tiles, 128), F32),
        ]
        + [pltpu.VMEM((6 * tiles, 128), F32)] * ITERS
        + [
            pltpu.VMEM((3 * tiles, 128), F32),
            pltpu.VMEM((ITERS, 3 * tiles, 128), F32),
            pltpu.VMEM((ITERS, 3 * tiles, 128), F32),
            pltpu.VMEM((6 * tiles, 128), F32),
            pltpu.VMEM((3 * tiles, 128), F32),
            pltpu.VMEM((3 * tiles, 128), F32),
            pltpu.VMEM((tiles, 256, 384), jnp.bfloat16),
            pltpu.VMEM((2 * tiles, 6 * tiles), jnp.bfloat16),
            pltpu.VMEM((128, 128), F32),
            pltpu.VMEM((128, 128), F32),
            pltpu.VMEM((2, inner, 1, 128), F32),
            pltpu.VMEM((2, outer, 1, 128), F32),
            pltpu.SemaphoreType.DMA((ring_count,)),
            pltpu.SemaphoreType.DMA((ring_count,)),
            pltpu.SemaphoreType.DMA((sum_count,)),
            pltpu.SemaphoreType.DMA((sum_count,)),
        ],
        compiler_params=pltpu.CompilerParams(
            collective_id=0, has_side_effects=True, vmem_limit_bytes=60 * 1024 * 1024
        ),
        name="solve",
    )(
        positions,
        polar.reshape(tiles, 128),
        field_ext,
        tile_atom.reshape(tiles, 128),
        tile_list.T,
        image_shift.transpose(2, 0, 1),
        tile_list.T,
    )

    return pl.pallas_call(
        atom_order_kernel,
        out_shape=(shape(3, atoms), shape(3, atoms)),
        in_specs=[vmem] * 3,
        out_specs=(vmem,) * 2,
        name="atom_order",
    )(*(pltpu.with_memory_space_constraint(value, pltpu.VMEM) for value in (x, r, slot)))


def solution(mesh):
    both = ("rep", "gx")
    return jax.shard_map(
        functools.partial(on_device, mesh.shape["gx"]),
        mesh=mesh,
        in_specs=(
            P(None, both),
            P(both),
            P(None, both),
            P(both),
            P(both, None),
            P(None, both, None),
        ),
        out_specs=(P(None, both), P(None, both)),
        check_vma=False,
    )
```

```python
import functools
import math

import jax
import jax.numpy as jnp
from jax import lax
from jax.experimental import pallas as pl
from jax.experimental.pallas import tpu as pltpu
from jax.sharding import PartitionSpec as P

ITERS = 4
MESH = pl.DeviceIdType.MESH
THOLE = 0.39
F32 = jnp.float32
ROWS = 8


def lanes(index):
    return slice(index * 128, (index + 1) * 128)


def gathered(slot, rows_at, count, steps):
    blocks = []
    for start in range(0, slot.shape[0], 8):
        index = slot[start : start + 8]
        high = lax.shift_right_logical(index, 7)
        low = jnp.bitwise_and(index, 127)

        def pick(step, found):
            hit = high == step
            return tuple(
                jnp.where(
                    hit,
                    jnp.take_along_axis(jnp.broadcast_to(row, (8, 128)), low, axis=1),
                    old,
                )
                for row, old in zip(rows_at(step), found)
            )

        zero = jnp.zeros((8, 128), F32)
        blocks.append(lax.fori_loop(0, steps, pick, (zero,) * count, unroll=True))
    return blocks


def inverse_order(atom):
    tiles = atom.shape[0]
    high_ids = lax.broadcasted_iota(jnp.int32, (tiles, 128), 0)
    low_ids = lax.broadcasted_iota(jnp.int32, (128, 128), 0)
    lane_ids = lax.broadcasted_iota(jnp.int32, (tiles, 128), 1).astype(F32)
    high = lax.shift_right_logical(atom, 7)
    low = jnp.bitwise_and(atom, 127)
    total = None
    for pair in range(0, tiles, 2):
        left, right = [], []
        for step in (pair, pair + 1):
            hot = high_ids == high[step : step + 1]
            left.append(
                jnp.concatenate(
                    [jnp.where(hot, float(step), 0.0), jnp.where(hot, lane_ids, 0.0)], axis=0
                )
            )
            right.append(jnp.where(low_ids == low[step : step + 1], 1.0, 0.0))
        term = lax.dot_general(
            jnp.concatenate(left, axis=1).astype(jnp.bfloat16),
            jnp.concatenate(right, axis=1).astype(jnp.bfloat16),
            (((1,), (1,)), ((), ())),
            preferred_element_type=F32,
        )
        total = term if total is None else total + term
    return (total[:tiles] * 128.0 + total[tiles:]).astype(jnp.int32)


def atom_order_kernel(x_ref, r_ref, slot_ref, dipoles_ref, residual_ref):
    tiles = slot_ref.shape[0]

    def rows_at(step):
        return [ref[pl.ds(c * tiles + step, 1), :] for ref in (x_ref, r_ref) for c in range(3)]

    for block, found in enumerate(gathered(slot_ref[...], rows_at, 6, tiles)):
        for c in range(3):
            for h in range(8):
                dipoles_ref[c : c + 1, lanes(8 * block + h)] = found[c][h : h + 1, :]
                residual_ref[c : c + 1, lanes(8 * block + h)] = found[3 + c][h : h + 1, :]


def pair_tensor(left, right, diagonal):
    dx = right[0] - left[0]
    dy = right[1] - left[1]
    dz = right[2] - left[2]
    square = dx * dx + dy * dy + dz * dz
    if diagonal is not None:
        square = jnp.where(diagonal, 1.0, square)
    inv = lax.rsqrt(square)
    minus_u = square * (square * inv) * (left[3] * right[3])
    decay = jnp.exp(minus_u)
    inv_cube = inv * (inv * inv)
    rest = 1.0 - decay
    g3 = rest * inv_cube
    if diagonal is not None:
        g3 = jnp.where(diagonal, 0.0, g3)
    damped = (rest + minus_u * decay) * inv_cube
    scale = (damped * lax.rsqrt(damped)) * (inv * math.sqrt(3.0))
    return (dx * scale, dy * scale, dz * scale), g3


def along(e, m):
    share = e[0] * m[0] + e[1] * m[1] + e[2] * m[2]
    return (e[0] * share, e[1] * share, e[2] * share)


def solve_kernel(
    group,
    inner,
    pos_ref,
    polar_ref,
    field_ref,
    atom_ref,
    list_ref,
    shift_ref,
    lines_ref,
    x_ref,
    r_ref,
    slot_ref,
    inv_alpha_ref,
    own_t,
    pair_t,
    part,
    cols_a,
    cols_b,
    cols_c,
    cols_d,
    win_p,
    win_0,
    win_1,
    win_2,
    win_3,
    top,
    ret_out,
    ret_in,
    right_rows,
    own_rows,
    left_rows,
    scalar_t,
    hot,
    colmat,
    gram,
    sums_1,
    sums_2,
    ring_send,
    ring_recv,
    sum_send,
    sum_recv,
):
    tiles = atom_ref.shape[0]
    me = lax.axis_index("gx")
    outer = group // inner
    row, col = me // inner, me % inner
    after = lax.rem(me + 1, group)
    before = lax.rem(me + group - 1, group)
    peers_1 = [row * inner + lax.rem(col + d, inner) for d in range(1, inner)]
    peers_2 = [lax.rem(row + d, outer) * inner + col for d in range(1, outer)]
    wins = (win_0, win_1, win_2, win_3)
    cols = (cols_a, cols_b, cols_c, cols_d)

    barrier = pltpu.get_barrier_semaphore()
    everyone = [after, before] + peers_1 + peers_2
    for peer in everyone:
        pl.semaphore_signal(barrier, inc=1, device_id={"gx": peer}, device_id_type=MESH)

    def ring_copy(src, dst, index, peer):
        return pltpu.make_async_remote_copy(
            src_ref=src,
            dst_ref=dst,
            send_sem=ring_send.at[index],
            recv_sem=ring_recv.at[index],
            device_id={"gx": peer},
            device_id_type=MESH,
        )

    def sum_copies(which, stage):
        buf = sums_1 if stage == 0 else sums_2
        at = col if stage == 0 else row
        peers = peers_1 if stage == 0 else peers_2
        base = which * (inner + outer) + stage * inner
        return [
            pltpu.make_async_remote_copy(
                src_ref=buf.at[which, at],
                dst_ref=buf.at[which, at],
                send_sem=sum_send.at[base + d],
                recv_sem=sum_recv.at[base + d],
                device_id={"gx": peer},
                device_id_type=MESH,
            )
            for d, peer in enumerate(peers)
        ]

    def sum_start(which, stage, value):
        buf = sums_1 if stage == 0 else sums_2
        buf[which, pl.ds(col if stage == 0 else row, 1)] = value[None]
        for copy in sum_copies(which, stage):
            copy.start()

    def sum_finish(which, stage):
        for copy in sum_copies(which, stage):
            copy.wait()
        buf = sums_1 if stage == 0 else sums_2
        total = buf[which, 0]
        for d in range(1, inner if stage == 0 else outer):
            total = total + buf[which, d]
        return total

    def inner_rows(a, b):
        return jnp.sum(a * b, axis=0, keepdims=True)

    sub_ids = lax.broadcasted_iota(jnp.int32, (16, 128), 0)
    lane_ids = lax.broadcasted_iota(jnp.int32, (16, 128), 1)

    def packed_sums(stack):
        totals = jnp.sum(stack, axis=1, keepdims=True)
        return jnp.sum(jnp.where(sub_ids == lane_ids, totals, 0.0), axis=0, keepdims=True)

    def unpacked(sums):
        gram[...] = jnp.broadcast_to(sums, (128, 128)).T

    def rows_at(ref):
        def rows(step):
            places = pl.ds(pl.multiple_of(step * 128, 128), 128)
            return [ref[c : c + 1, places] for c in range(3)]

        return rows

    def place_rows(step):
        return rows_at(pos_ref)(step) + [polar_ref[pl.ds(step, 1), :]]

    for block, found in enumerate(gathered(atom_ref[...], place_rows, 4, tiles)):
        for c in range(3):
            at = c * tiles + 8 * block
            win_p[at : at + 8, :] = found[c]
        at = 3 * tiles + 8 * block
        win_p[at : at + 8, :] = lax.rsqrt(found[3])
        inv_alpha_ref[8 * block : 8 * block + 8, :] = 1.0 / found[3]

    steps = 128 // ROWS

    def spread(buf, ref, index, count):
        for c in range(count):
            line = ref[pl.ds(c * tiles + index, 1), :]
            buf[:, c] = jnp.broadcast_to(line, (128, 128)).T.reshape(steps, ROWS, 128)

    def right_lines(n, vector):
        first = n + jnp.where(n >= tiles, 3 * tiles, 0)
        lines = [win_p[pl.ds(first + c * tiles, 1), :] for c in range(4)]
        if vector is not None:
            lines = [lines[c] + vector[c] for c in range(3)] + lines[3:]
        lines[3] = lines[3] * (-THOLE)
        return [jnp.broadcast_to(line, (2 * ROWS, 128)) for line in lines]

    sub_16 = lax.broadcasted_iota(jnp.int32, (2 * ROWS, 128), 0)
    lane_16 = lax.broadcasted_iota(jnp.int32, (2 * ROWS, 128), 1)
    sub_8 = lax.broadcasted_iota(jnp.int32, (ROWS, 128), 0)
    lines_of = [jnp.logical_or(sub_8 == c, sub_8 == c + 3) for c in range(3)]
    halves = [jnp.logical_or(sub_16 == c, sub_16 == c + 3) for c in range(3)]

    def tensors(t, cols, right, diagonal, where, place):
        def block(i, carry):
            left = [cols[pl.ds(2 * i, 2), c].reshape(2 * ROWS, 128) for c in range(4)]
            same = sub_16 + i * (2 * ROWS) == lane_16 if diagonal else None
            e, g3 = pair_tensor(left, right, same)
            for c in range(3):
                where(t, i, c, e[c].reshape(2, ROWS, 128))
            high = g3.astype(jnp.bfloat16)
            low = (g3 - high.astype(F32)).astype(jnp.bfloat16)
            at = pl.multiple_of(i * (2 * ROWS), 2 * ROWS)
            scalar_t[t, pl.ds(at, 2 * ROWS), lanes(place)] = high
            scalar_t[t, pl.ds(128 + at, 2 * ROWS), lanes(place)] = low
            return carry

        lax.fori_loop(0, steps // 2, block, 0, unroll=True)

    def own_tensors(t, cols):
        def where(t, i, c, value):
            own_t[t, pl.ds(2 * i, 2), c] = value

        tensors(t, cols, right_lines(t, None), True, where, 2)

    def split_lines(lines):
        wide = jnp.where(halves[0], lines[0], jnp.where(halves[1], lines[1], lines[2]))
        high = wide.astype(jnp.bfloat16).astype(F32)
        return jnp.where(sub_16 < 3, high, wide - high).astype(jnp.bfloat16)

    last = me == group - 1

    def pair_tensors(t, cols):
        for e in range(2):
            n = list_ref[e + 1, t]
            wrap = jnp.where(jnp.logical_and(n >= tiles, last), 4.0 * group, 0.0)
            vector = (
                wrap,
                shift_ref[e + 1, 0, t].astype(F32) * 128.0,
                shift_ref[e + 1, 1, t].astype(F32) * (2.0 * tiles),
            )

            def where(t, i, c, value, e=e):
                pair_t[t, e, pl.ds(2 * i, 2), c] = value

            tensors(t, cols, right_lines(n, vector), False, where, e)

    def own_fields(win, first=0, stop=tiles):
        def body(t, carry):
            m = [
                jnp.broadcast_to(win[pl.ds(c * tiles + t, 1), :], (ROWS, 128))
                for c in range(3)
            ]

            def block(i, inside):
                tensor = [own_t[t, i, c] for c in range(3)]
                for c, value in enumerate(along(tensor, m)):
                    part[t, i, c] = value
                return inside

            lax.fori_loop(0, steps, block, 0, unroll=True)
            return carry

        lax.fori_loop(first, stop, body, 0)

    def in_turns(ref, count, work, turns, first=0, stop=tiles):
        for slot, buf in enumerate(cols[0:2]):
            spread(buf, ref, first + slot, count)

        def body(u, carry):
            t = first + 2 * turns * u
            for turn in range(turns):
                now, later = 2 * (turn % 2), 2 * ((turn + 1) % 2)
                for step in range(2):
                    ahead = lax.rem(t + 2 * turn + 2 + step, tiles)
                    spread(cols[later + step], ref, ahead, count)
                    work(t + 2 * turn + step, cols[now + step])
            return carry

        lax.fori_loop(0, (stop - first) // (2 * turns), body, 0)

    def right_fields(win, with_own):
        sources = 3 if with_own else 2

        def work(t, cols):
            lines = [
                jnp.broadcast_to(win[pl.ds(c * tiles + t, 1), :], (2 * ROWS, 128))
                for c in range(3)
            ]
            split = split_lines(lines)
            scalar = jnp.dot(
                jnp.concatenate([split, split], axis=1), scalar_t[t], preferred_element_type=F32
            )[0:ROWS]

            def block(i, sums):
                m = [cols[i, c] for c in range(3)]
                new = []
                for e in range(sources):
                    tensor = [own_t[t, i, c] if e == 2 else pair_t[t, e, i, c] for c in range(3)]
                    new += list(along(tensor, m))
                return tuple(a + b for a, b in zip(sums, new))

            zeros = (jnp.zeros((ROWS, 128), F32),) * (3 * sources)
            sums = lax.fori_loop(0, steps, block, zeros, unroll=True)
            for c in range(3):
                less = [jnp.where(lines_of[c], scalar[:, lanes(e)], 0.0) for e in range(3)]
                own = sums[6 + c] - less[2] if with_own else -less[2]
                own_rows[pl.ds(c * tiles + t, 1), :] = jnp.sum(own, axis=0, keepdims=True)
                for e in range(2):
                    right_rows[pl.ds(tiles * (2 * c + e) + t, 1), :] = jnp.sum(
                        sums[3 * e + c] - less[e], axis=0, keepdims=True
                    )

        in_turns(win, 3, work, 4)
        rows = right_rows[...]
        rows = jnp.concatenate(
            [rows[2 * tiles * c : 2 * tiles * (c + 1)] for c in range(3)], axis=1
        )
        first = rows.astype(jnp.bfloat16)
        rows = rows - first.astype(F32)
        second = rows.astype(jnp.bfloat16)
        third = (rows - second.astype(F32)).astype(jnp.bfloat16)
        split = jnp.concatenate([first, second, third], axis=0)
        total = jnp.dot(hot[...], split, preferred_element_type=F32)
        return [
            jnp.concatenate([half[:, lanes(c)] for c in range(3)], axis=0)
            for half in (total[0:tiles], total[tiles : 2 * tiles])
        ]

    full_lane = lax.broadcasted_iota(jnp.int32, (128, 128), 1)

    def gather_column(t):
        now = colmat[...]
        for c in range(3):
            total = jnp.sum(part[t, :, c].reshape(128, 128), axis=1, keepdims=True)
            now = jnp.where(full_lane == c * tiles + t, total, now)
        colmat[...] = now

    def left_fields(win, with_part):
        def one(t):
            gather_column(lax.rem(t + tiles - 1, tiles))
            m = []
            for e in range(2):
                n = list_ref[e + 1, t]
                first = n + jnp.where(n >= tiles, 2 * tiles, 0)
                m.append(
                    [
                        jnp.broadcast_to(win[pl.ds(first + c * tiles, 1), :], (2 * ROWS, 128))
                        for c in range(3)
                    ]
                )
            scalar = lax.dot_general(
                jnp.concatenate([split_lines(lines) for lines in m], axis=1),
                scalar_t[t, :, 0:256],
                (((1,), (1,)), ((), ())),
                preferred_element_type=F32,
            )[0:ROWS]
            scalar = scalar[:, lanes(0)] + scalar[:, lanes(1)]
            for c in range(3):
                left_rows[pl.ds(c * tiles + t, 1), :] = jnp.sum(
                    jnp.where(lines_of[c], scalar, 0.0), axis=0, keepdims=True
                )
            m = [[line[0:ROWS] for line in lines] for lines in m]

            def block(i, inside):
                sums = [part[t, i, c] for c in range(3)] if with_part else None
                for e in range(2):
                    tensor = [pair_t[t, e, i, c] for c in range(3)]
                    new = along(tensor, m[e])
                    sums = new if sums is None else [a + b for a, b in zip(sums, new)]
                for c in range(3):
                    part[t, i, c] = sums[c]
                return inside

            lax.fori_loop(0, steps, block, 0, unroll=True)

        def body(u, carry):
            for step in range(8):
                one(8 * u + step)
            return carry

        lax.fori_loop(0, tiles // 8, body, 0)
        gather_column(tiles - 1)
        return colmat[...].T[0 : 3 * tiles] - left_rows[...]

    in_turns(win_p, 4, own_tensors, 2, 0, tiles // 4)

    pl.semaphore_wait(barrier, len(everyone))
    own_p, own_v = 4 * tiles, 3 * tiles
    halo_p = ring_copy(win_p.at[0:own_p], win_p.at[own_p : 2 * own_p], 0, before)
    halo_p.start()

    for block, found in enumerate(gathered(atom_ref[...], rows_at(field_ref), 3, tiles)):
        for c in range(3):
            at = c * tiles + 8 * block
            win_0[at : at + 8, :] = found[c]

    rhs = win_0[0 : 3 * tiles, :]
    inv_alpha = inv_alpha_ref[...]
    inv_alpha_3 = jnp.concatenate([inv_alpha] * 3, axis=0)
    colmat[...] = jnp.zeros((128, 128), F32)
    gram[...] = jnp.zeros((128, 128), F32)
    gram[0:1, :] = inner_rows(rhs, rhs)
    gram[1:2, :] = inner_rows(rhs, rhs * inv_alpha_3)

    halos = [
        ring_copy(win.at[0:own_v], win.at[own_v : 2 * own_v], 1 + k, before)
        for k, win in enumerate(wins)
    ]
    returns = [
        ring_copy(ret_out.at[k], ret_in.at[k], 1 + ITERS + k, after) for k in range(ITERS)
    ]
    halos[0].start()
    sum_start(0, 0, packed_sums(gram[0:16, :]))

    in_turns(win_p, 4, own_tensors, 4, tiles // 4, tiles)
    own_fields(win_0)

    tile_ids = lax.broadcasted_iota(jnp.int32, (2 * tiles, tiles), 0)
    marks = [jnp.where(lines_ref[e : e + 1, :] == tile_ids, 1.0, 0.0) for e in (1, 2)]
    hot[...] = jnp.concatenate(marks * 3, axis=1).astype(jnp.bfloat16)

    halo_p.wait()
    in_turns(win_p, 4, pair_tensors, 2)
    sum_start(0, 1, sum_finish(0, 0))

    def own_vector(k):
        return wins[k][0:own_v, :]

    pair_index = {}

    def keep(key, line):
        index = pair_index[key] = len(pair_index)
        gram[index : index + 1, :] = line

    centre = None
    for k in range(ITERS):
        final = k + 1 == ITERS
        if k > 0:
            keep((k, k), inner_rows(own_vector(k), own_vector(k)))
            halos[k].start()
            for j in range(k):
                keep((j, k), inner_rows(own_vector(j), own_vector(k)))
        kept, sent = right_fields(wins[k], final)
        ret_out[k] = sent
        if k > 0 and not final:
            own_fields(wins[k], 0, 4)
        if final:
            now = own_vector(k)
            line = inner_rows(now, shifted * now - (own_rows[...] + 2.0 * kept))
        kept = kept + own_rows[...]
        returns[k].start()
        if k > 0 and not final:
            own_fields(wins[k], 4, tiles)
        halos[k].wait()
        if final:
            line = line - 2.0 * inner_rows(wins[k][own_v : 2 * own_v, :], sent)
            keep((k, k + 1), line)
            sum_start(1, 0, packed_sums(gram[0:16, :]))
        field = left_fields(wins[k], not final) + kept
        if k == 0:
            unpacked(sum_finish(0, 1))
            centre = gram[1:2, :] / gram[0:1, :]
            gram[...] = jnp.zeros((128, 128), F32)
            keep((0, 0), inner_rows(rhs, rhs))
            shifted = jnp.concatenate([inv_alpha - centre] * 3, axis=0)
        if final:
            slot_ref[...] = inverse_order(atom_ref[...])
            sum_start(1, 1, sum_finish(1, 0))
        returns[k].wait()
        new = shifted * own_vector(k) - (field + ret_in[k])
        if final:
            top[...] = new
        else:
            wins[k + 1][0:own_v, :] = new

    unpacked(sum_finish(1, 1))
    vectors = [own_vector(k) for k in range(ITERS)] + [top[...]]
    for j in range(ITERS - 1):
        pair_index[(j, ITERS)] = pair_index[(j + 1, ITERS - 1)]

    def entry(a, b):
        index = pair_index[(min(a, b), max(a, b))]
        return gram[index : index + 1, :]

    def form(a, b):
        terms = [p * (q * entry(i, j)) for i, p in enumerate(a) for j, q in enumerate(b)]
        while len(terms) > 1:
            terms = [sum(terms[i + 1 : i + 2], terms[i]) for i in range(0, len(terms), 2)]
        return terms[0]

    def plus(a, scale, b):
        out = []
        for i in range(max(len(a), len(b))):
            term = scale * b[i] if i < len(b) else None
            if i < len(a):
                out.append(a[i] if term is None else a[i] + term)
            else:
                out.append(term)
        return out

    one = jnp.ones((1, 128), F32)
    x_coef = []
    r_coef = [one]
    d_coef = [one]
    norm_now = form(r_coef, r_coef)
    for iteration in range(ITERS):
        applied = [centre * v for v in d_coef] + [0.0 * one]
        applied = [
            applied[i] + d_coef[i - 1] if i > 0 else applied[i] for i in range(len(applied))
        ]
        step = norm_now / form(d_coef, applied)
        x_coef = plus(x_coef, step, d_coef)
        r_coef = plus(r_coef, -step, applied)
        if iteration + 1 < ITERS:
            norm_next = form(r_coef, r_coef)
            d_coef = plus(r_coef, norm_next / norm_now, d_coef)
            norm_now = norm_next

    for out_ref, coef in ((x_ref, x_coef), (r_ref, r_coef)):
        total = None
        for j, value in enumerate(coef):
            term = value * vectors[j]
            total = term if total is None else total + term
        out_ref[...] = total


def on_device(group, positions, polar, field_ext, tile_atom, tile_list, image_shift):
    atoms = tile_atom.shape[0]
    tiles = tile_list.shape[0]
    inner = 16 if group % 16 == 0 else 2
    outer = group // inner
    steps = 128 // ROWS
    vmem = pl.BlockSpec(memory_space=pltpu.VMEM)
    smem = pl.BlockSpec(memory_space=pltpu.SMEM)

    def shape(*dims, dtype=F32):
        return jax.ShapeDtypeStruct(dims, dtype)

    sum_count = 2 * (inner + outer)
    ring_count = 1 + 2 * ITERS
    x, r, slot = pl.pallas_call(
        functools.partial(solve_kernel, group, inner),
        out_shape=(
            pltpu.VMEM((3 * tiles, 128), F32),
            pltpu.VMEM((3 * tiles, 128), F32),
            pltpu.VMEM((tiles, 128), jnp.int32),
        ),
        in_specs=[vmem] * 4 + [smem] * 2 + [vmem],
        out_specs=(vmem,) * 3,
        scratch_shapes=[
            pltpu.VMEM((tiles, 128), F32),
            pltpu.VMEM((tiles, steps, 3, ROWS, 128), F32),
            pltpu.VMEM((tiles, 2, steps, 3, ROWS, 128), F32),
            pltpu.VMEM((tiles, steps, 3, ROWS, 128), F32),
            pltpu.VMEM((steps, 4, ROWS, 128), F32),
            pltpu.VMEM((steps, 4, ROWS, 128), F32),
            pltpu.VMEM((steps, 4, ROWS, 128), F32),
            pltpu.VMEM((steps, 4, ROWS, 128), F32),
            pltpu.VMEM((8 * tiles, 128), F32),
        ]
        + [pltpu.VMEM((6 * tiles, 128), F32)] * ITERS
        + [
            pltpu.VMEM((3 * tiles, 128), F32),
            pltpu.VMEM((ITERS, 3 * tiles, 128), F32),
            pltpu.VMEM((ITERS, 3 * tiles, 128), F32),
            pltpu.VMEM((6 * tiles, 128), F32),
            pltpu.VMEM((3 * tiles, 128), F32),
            pltpu.VMEM((3 * tiles, 128), F32),
            pltpu.VMEM((tiles, 256, 384), jnp.bfloat16),
            pltpu.VMEM((2 * tiles, 6 * tiles), jnp.bfloat16),
            pltpu.VMEM((128, 128), F32),
            pltpu.VMEM((128, 128), F32),
            pltpu.VMEM((2, inner, 1, 128), F32),
            pltpu.VMEM((2, outer, 1, 128), F32),
            pltpu.SemaphoreType.DMA((ring_count,)),
            pltpu.SemaphoreType.DMA((ring_count,)),
            pltpu.SemaphoreType.DMA((sum_count,)),
            pltpu.SemaphoreType.DMA((sum_count,)),
        ],
        compiler_params=pltpu.CompilerParams(
            collective_id=0, has_side_effects=True, vmem_limit_bytes=60 * 1024 * 1024
        ),
        name="solve",
    )(
        positions,
        polar.reshape(tiles, 128),
        field_ext,
        tile_atom.reshape(tiles, 128),
        tile_list.T,
        image_shift.transpose(2, 0, 1),
        tile_list.T,
    )

    return pl.pallas_call(
        atom_order_kernel,
        out_shape=(shape(3, atoms), shape(3, atoms)),
        in_specs=[vmem] * 3,
        out_specs=(vmem,) * 2,
        name="atom_order",
    )(*(pltpu.with_memory_space_constraint(value, pltpu.VMEM) for value in (x, r, slot)))


def solution(mesh):
    both = ("rep", "gx")
    return jax.shard_map(
        functools.partial(on_device, mesh.shape["gx"]),
        mesh=mesh,
        in_specs=(
            P(None, both),
            P(both),
            P(None, both),
            P(both),
            P(both, None),
            P(None, both, None),
        ),
        out_specs=(P(None, both), P(None, both)),
        check_vma=False,
    )
```
